32 devices in a mesh: lat: 4 (over z), rad: 8 (over y, x, core).
Axes of the slice: x: 2, y: 2, z: 4, core: 2. Of those that a mesh axis runs over, the one named last changes fastest.
Arguments:
- positions: float32 [4096, 3, 128], P(('lat', 'rad')), may hold values from 0 to 1
- fields: bfloat16 [4096, 16, 128], P(('lat', 'rad')), may hold values from -6 to 6
- velocity: float32 [81, 8192], P(None, ('lat', 'rad')), may hold values from -3 to 3
- counts: int32 [32], P(('lat', 'rad')), may hold values from 1 to 128, as said below
- elements: int32 [3, 4096], P(None, ('lat', 'rad')), may hold values from 0 to 255
- routes: int32 [2, 4096], P(None, ('lat', 'rad')), may hold values from 0 to 239, as said below
Outputs:
- moved: float32 [7680, 3, 128], P(('lat', 'rad'))
- projected: float32 [27, 16, 8192], P(None, None, ('lat', 'rad'))
The draws below stay inside these ranges and needn't reach their ends.
Inputs may be any that keep to these rules, and one draw needn't show every extreme that they name: counts[d] is at most 128 and equals 128 on some device. Both rows code destinations as in the reference program. routes[0] differs between any two blocks of one device; routes[1] differs between any two blocks that routes[0] sends to the same device.
All inputs are finite; a program needn't handle non-finite values.
Results may differ from the reference program's by a relative error of at most 0.0003.
Values sent between devices are 32-bit elements; how exact they have to be, the bound alone decides.
A program may use at most 64 MiB of HBM per device.

```python
import jax
import jax.numpy as jnp
from jax import lax

BLOCK = 128
FIELDS = 16
MB = 128
NE = 256
CAP = 10
SLOTS = 240
BLOCKS = 4096
ELEMS = 8192
N_LAT = 4
N_RAD = 8
DEVICES = 32


def draw_counts(key, part):
    keys = jax.random.split(jax.random.fold_in(key, 11), 2)
    lowest = max(1, MB // 4)
    drawn = jax.random.randint(keys[0], (DEVICES,), lowest, MB + 1)
    fullest = jax.random.randint(keys[1], (), 0, DEVICES)
    return jnp.where(jnp.arange(DEVICES) == fullest, MB, drawn).astype(jnp.int32)


def shuffled(key, height, width):
    scores = jax.random.randint(key, (height, width), 0, 1 << 20) * width + jnp.arange(width)[None, :]
    return jnp.argsort(scores, axis=1).astype(jnp.int32)


def draw_routes(key, part):
    keys = jax.random.split(jax.random.fold_in(key, 23), 2)
    first_route = shuffled(keys[0], DEVICES, SLOTS)[:, :MB].reshape(-1)
    home = jnp.arange(DEVICES * MB, dtype=jnp.int32) // MB
    lat_step = first_route // (N_RAD * CAP)
    mid_rad = first_route // CAP % N_RAD
    mid_place = first_route % CAP
    middle = (home // N_RAD + lat_step - 1) % N_LAT * N_RAD + mid_rad
    arrival = (lat_step * N_RAD + home % N_RAD) * CAP + mid_place
    second_route = shuffled(keys[1], DEVICES, SLOTS)[middle, arrival]
    return jnp.stack([first_route, second_route]).astype(jnp.int32)


def set_ends(result, key, smallest, top_value):
    place = [jax.random.randint(jax.random.fold_in(key, axis), (), 0, length) for axis, length in enumerate(result.shape)]
    longest = result.shape.index(max(result.shape))
    next_to = place[:longest] + [(place[longest] + 1) % result.shape[longest]] + place[longest + 1:]
    return result.at[tuple(place)].set(smallest).at[tuple(next_to)].set(top_value)


def block_levels(key, shape, cuts, least, top_value):
    loudness = 1.0
    for position, blocks in cuts:
        steps = jax.random.uniform(jax.random.fold_in(jax.random.fold_in(key, 6), position), (blocks,), jnp.float32, least / len(cuts), top_value / len(cuts))
        loudness = loudness * jnp.repeat(jnp.exp(steps), shape[position] // blocks).reshape((-1,) + (1,) * (len(shape) - 1 - position))
    return loudness


def bell_draw(rng, dims, deviation, limit, pieces=(), kind=jnp.bfloat16):
    result = deviation * jax.random.normal(rng, dims, jnp.float32)
    if pieces:
        result = result * block_levels(rng, dims, pieces, -0.22, 0.18)
    return jnp.clip(result, -limit, limit).astype(kind)


def setup_inputs(seed: int = 0) -> dict:
    seeds = jax.random.split(jax.random.key(seed), 7)
    return {
        "positions": jnp.clip(1.0 * jax.random.uniform(seeds[0], (BLOCKS, 3, BLOCK), jnp.float32) ** block_levels(seeds[0], (BLOCKS, 3, BLOCK), ((0, 32),), -0.2, 0.2), 0.0, 1.0),
        "fields": bell_draw(seeds[1], (BLOCKS, FIELDS, BLOCK), 1.0, 6.0, ((0, 32),)),
        "velocity": bell_draw(seeds[2], (81, ELEMS), 0.5, 3.0, ((1, 32),), jnp.float32),
        "counts": draw_counts(jax.random.fold_in(seeds[6], 71), 0),
        "elements": set_ends(jax.random.randint(seeds[4], (3, BLOCKS), 0, NE), jax.random.fold_in(seeds[4], 1), 0, NE - 1).astype(jnp.int32),
        "routes": draw_routes(jax.random.fold_in(seeds[6], 71), 0),
    }


time_step = 0.4
exact = lax.Precision.HIGHEST


def lagrange(coord):
    first_node = 2.0 * (coord - 0.5) * (coord - 1.0)
    middle_node = -4.0 * coord * (coord - 1.0)
    last_node = 2.0 * coord * (coord - 0.5)
    return jnp.stack([first_node, middle_node, last_node], axis=0)


def basis(points):
    along_x = lagrange(points[:, 0, :])
    along_y = lagrange(points[:, 1, :])
    along_z = lagrange(points[:, 2, :])
    table = along_x[:, None, None] * along_y[None, :, None] * along_z[None, None, :]
    return jnp.moveaxis(table.reshape(27, points.shape[0], points.shape[2]), 0, 1)


def speed(columns, points):
    coefficients = columns.T.reshape(points.shape[0], 3, 27)
    return jnp.einsum("scn,snb->scb", coefficients, basis(points), precision=exact)


def reference(positions, fields, velocity, counts, elements, routes):
    devices = N_LAT * N_RAD
    total = positions.shape[0]
    width = positions.shape[2]
    order = jnp.arange(total, dtype=jnp.int32)
    home = order // MB
    valid = (order % MB) < counts[home]
    lat_step = routes[0] // (N_RAD * CAP)
    mid_rad = (routes[0] // CAP) % N_RAD
    mid_lat = (home // N_RAD + lat_step - 1) % N_LAT
    middle = mid_lat * N_RAD + mid_rad
    next_step = routes[1] // (N_RAD * CAP)
    final_rad = (routes[1] // CAP) % N_RAD
    final_place = routes[1] % CAP
    final = ((mid_lat + next_step - 1) % N_LAT) * N_RAD + final_rad
    out_rows = (final * SLOTS + (next_step * N_RAD + mid_rad) * CAP + final_place).astype(jnp.int32)
    start_cols = (home * NE + elements[0]).astype(jnp.int32)
    middle_cols = (middle * NE + elements[1]).astype(jnp.int32)
    final_cols = (final * NE + elements[2]).astype(jnp.int32)

    def advance(block_set):
        points, fractions, start, middle_col = block_set
        first_speed = speed(jnp.take(velocity, start, axis=1), points)
        midway = points + (0.5 * time_step) * first_speed
        landed = points + time_step * speed(jnp.take(velocity, middle_col, axis=1), midway)
        shapes = basis(landed)
        moments = jnp.einsum("snb,sfb->snf", shapes, fractions.astype(jnp.float32), precision=exact)
        return landed, moments, jnp.sum(shapes * shapes, axis=2)

    landed, moments, weights = lax.map(advance, (positions.reshape(devices, MB, 3, width), fields.reshape(devices, MB, fields.shape[1], width), start_cols.reshape(devices, MB), middle_cols.reshape(devices, MB)))
    landed = landed.reshape(total, 3, width)
    moments = moments.reshape(total, 27, fields.shape[1])
    weights = weights.reshape(total, 27)
    live = valid.astype(jnp.float32)
    moved = jnp.zeros((devices * SLOTS, 3, width), jnp.float32).at[out_rows].set(landed * live[:, None, None])
    totals = jax.ops.segment_sum(moments * live[:, None, None], final_cols, num_segments=devices * NE)
    summed = jax.ops.segment_sum(weights * live[:, None], final_cols, num_segments=devices * NE)
    projected = totals / (1.0 + summed[:, :, None])
    return moved, jnp.transpose(projected, (1, 2, 0))
```

```python
import functools

import jax
import jax.numpy as jnp
from jax import lax
from jax.experimental import pallas as pl
from jax.experimental.pallas import tpu as pltpu
from jax.sharding import PartitionSpec as P

time_step = 0.4
MESH = pl.DeviceIdType.MESH
LANES = 128
bf16, f32, i32 = jnp.bfloat16, jnp.float32, jnp.int32


def round_up(x, by):
    return -(-x // by) * by


def split(x):
    high = x.astype(bf16)
    low = (x - high.astype(f32)).astype(bf16)
    return high, low


def dot(a, b, dims):
    return lax.dot_general(a, b, (dims, ((), ())), preferred_element_type=f32)


def iota(shape, axis):
    return lax.broadcasted_iota(i32, shape, axis)


def mask(condition):
    return condition.astype(f32).astype(bf16)


def lagrange(s):
    return (2.0 * (s - 0.5) * (s - 1.0), -4.0 * s * (s - 1.0), 2.0 * s * (s - 0.5))


def advance(points_in, coefficients, base, out, scale, group):
    markers = base.shape[1]

    def step(g, carry):
        rows = pl.ds(pl.multiple_of(g * group, group), group)
        lx = lagrange(points_in[0, rows, :])
        ly = lagrange(points_in[1, rows, :])
        lz = lagrange(points_in[2, rows, :])
        sums = [None] * 3
        for i in range(3):
            inner = [None] * 3
            for j in range(3):
                for c in range(3):
                    n = c * 27 + 9 * i + 3 * j
                    line = (
                        coefficients[n : n + 1, :] * lz[0]
                        + coefficients[n + 1 : n + 2, :] * lz[1]
                        + coefficients[n + 2 : n + 3, :] * lz[2]
                    ) * ly[j]
                    inner[c] = line if inner[c] is None else inner[c] + line
            for c in range(3):
                term = inner[c] * lx[i]
                sums[c] = term if sums[c] is None else sums[c] + term
        for c in range(3):
            out[c, rows, :] = base[c, rows, :] + scale * sums[c]
        return carry

    lax.fori_loop(0, markers // group, step, 0)


def trip(
    n_lat, n_rad, capacity,
    counts, pos_in, vel_in, elements_in, routes_in, fld_in,
    fin_m, fin_e1, fin_e2,
    pos, vel, elements, routes, raw, wide, carried,
    start_points, midway, landed, coef, phi, table,
    tab_a, tab_e, tab_c, tab_m, points_m, midway_m, landed_m, coef_m0, coef_m1,
    request, asked, out_a, in_a, answer, answered, out_m,
    out_e1, in_e1, on_e1, out_e2, in_e2, on_e2,
    index_v, turn_v, index_s, turn_s,
    load_sem, send_sem, recv_sem,
):
    lat, rad = lax.axis_index("lat"), lax.axis_index("rad")
    slots = 3 * n_rad
    places = slots * capacity
    blocks, fields, markers = fld_in.shape
    n_vel, owned = vel.shape
    wide_places = points_m.shape[2]

    def load(index, source, target):
        copy = pltpu.make_async_copy(source, target, load_sem.at[index])
        copy.start()
        return copy

    load_routes = load(0, routes_in, routes)
    load_elements = load(1, elements_in, elements)
    load_vel = load(2, vel_in, vel)
    load_pos = load(3, pos_in, pos)
    load_fld = load(4, fld_in, raw)

    def partner(k, q, back):
        by = (1 - k) if back else (k - 1)
        return lax.rem(lat + by + n_lat, n_lat), q

    barrier = pltpu.get_barrier_semaphore()
    for k in range(3):

        def greet(dq, carry, k=k):
            q = lax.rem(rad + dq, n_rad)
            pl.semaphore_signal(
                barrier, inc=1, device_id=partner(k, q, False), device_id_type=MESH
            )
            return carry

        lax.fori_loop(1 if k == 1 else 0, n_rad, greet, 0)

    def exchange(phase, source, target, size, back=False):
        for k in (0, 2, 1):

            def send(dq, carry, k=k):
                q = lax.rem(rad + dq, n_rad)
                pltpu.make_async_remote_copy(
                    src_ref=source.at[pl.ds((k * n_rad + q) * size, size)],
                    dst_ref=target.at[pl.ds((k * n_rad + rad) * size, size)],
                    send_sem=send_sem.at[phase],
                    recv_sem=recv_sem.at[phase],
                    device_id=partner(k, q, back),
                    device_id_type=MESH,
                ).start()
                return carry

            lax.fori_loop(1 if k == 1 else 0, n_rad, send, 0)
        own = pl.ds((n_rad + rad) * size, size)
        pltpu.make_async_copy(source.at[own], target.at[own], recv_sem.at[phase]).start()

    def await_arrivals(phase, target, size):
        part = target.at[pl.ds(0, slots * size)]
        pltpu.make_async_copy(part, part, recv_sem.at[phase]).wait()

    def await_sends(phase, source, size):
        part = source.at[pl.ds(0, (slots - 1) * size)]
        pltpu.make_async_copy(part, part, send_sem.at[phase]).wait()

    def slot_of(place):
        return jnp.floor((place.astype(f32) + 0.5) * (1.0 / capacity)).astype(i32)

    def place_rows(out, source, indices, row, rows):
        def one(s, carry):
            for c in range(capacity):
                p = s * capacity + c
                at = jnp.clip(indices[row, p], 0, source.shape[0] - rows)
                out[pl.ds(p * rows, rows), :] = source[pl.ds(at, rows), :]
            return carry

        lax.fori_loop(0, slots, one, 0)

    zero_row = jnp.zeros((8, LANES), f32)
    tab_a[4 * blocks :, :] = jnp.zeros((tab_a.shape[0] - 4 * blocks, LANES), f32)
    tab_e[2 * blocks :, :] = jnp.zeros((tab_e.shape[0] - 2 * blocks, LANES), f32)
    in_a[4 * places :, :] = jnp.zeros((in_a.shape[0] - 4 * places, LANES), f32)
    in_e1[2 * places :, :] = jnp.zeros((in_e1.shape[0] - 2 * places, LANES), f32)
    in_e2[2 * places :, :] = jnp.zeros((in_e2.shape[0] - 2 * places, LANES), f32)
    answer[...] = jnp.zeros(answer.shape, f32)
    coef[...] = jnp.zeros(coef.shape, f32)

    load_routes.wait()
    load_elements.wait()
    route = jnp.where(iota((1, blocks), 1) < counts[0], routes[0:1, :], -1)
    slot = slot_of(route)
    sent_to = iota((slots, blocks), 0) == slot
    within = mask(iota((LANES, blocks), 0) == route - slot * capacity)
    for row, label in enumerate((elements[1:2, :], routes[1:2, :])):
        marked = jnp.where(sent_to, (label + 1).astype(f32), 0.0).astype(bf16)
        request[:, row, :] = dot(marked, within, ((1,), (1,)))
    pl.semaphore_wait(barrier, slots - 1)
    exchange(0, request, asked, 1)

    spread = mask(iota((index_v.shape[1], blocks), 0) == route)
    numbers = (iota((8, blocks), 1) - blocks).astype(f32).astype(bf16)
    holder = (dot(numbers, spread, ((1,), (1,))) + float(blocks)).astype(i32)
    index_v[0:1, :] = holder[0:1, :] * 4
    index_v[1:2, :] = holder[0:1, :] * 2
    index_v[2:3, 0:blocks] = jnp.maximum(route, 0)
    indices = pltpu.make_async_copy(index_v, index_s, load_sem.at[5])
    indices.start()

    load_vel.wait()
    vel_high, vel_low = split(vel[...])
    pick = mask(iota((owned, blocks), 0) == elements[0:1, :])
    coef[0:n_vel, :] = dot(vel_high, pick, ((1,), (0,))) + dot(vel_low, pick, ((1,), (0,)))
    tab_a[pl.ds(3, blocks, stride=4), :] = coef[...].T
    load_pos.wait()
    for c in range(3):
        tab_a[pl.ds(c, blocks, stride=4), :] = pos[c]
    indices.wait()
    place_rows(out_a, tab_a, index_s, 0, 4)
    exchange(1, out_a, in_a, 4 * capacity)

    for c in range(3):
        start_points[c] = pos[c].T
    advance(start_points, coef, start_points, midway, 0.5 * time_step, 16)

    own_slot = slot_of(iota((places, slots), 0))
    by_slot = mask(own_slot == iota((places, slots), 1))
    lane = iota((places, LANES), 0) - slot_of(iota((places, LANES), 0)) * capacity
    by_lane = lane == iota((places, LANES), 1)

    def label_column(row):
        lines = dot(by_slot, asked[:, row, :].astype(bf16), ((1,), (0,)))
        return jnp.sum(jnp.where(by_lane, lines, 0.0), axis=1, keepdims=True).astype(i32)

    await_arrivals(0, asked, 1)
    pick = mask(iota((places, owned), 1) + 1 == label_column(0))
    answer[0:places, 0:n_vel] = dot(pick, vel_high, ((1,), (1,))) + dot(
        pick, vel_low, ((1,), (1,))
    )
    exchange(2, answer, answered, capacity, back=True)

    turned = mask(iota((places, turn_v.shape[1]), 1) + 1 == label_column(1))
    numbers = (iota((8, places), 1) - places).astype(f32).astype(bf16)
    holder = (dot(numbers, turned, ((1,), (0,))) + float(places)).astype(i32)
    turn_v[0:1, :] = holder[0:1, :] * 4
    turn_v[1:2, :] = holder[0:1, :] * 2
    turns = pltpu.make_async_copy(turn_v, turn_s, load_sem.at[6])
    turns.start()

    load_fld.wait()
    wide[0 : blocks * fields, :] = raw[...].astype(f32).reshape(blocks * fields, markers)
    for f in range(fields):
        carried[pl.ds(f, markers, stride=fields), :] = wide[pl.ds(f, blocks, stride=fields), :].T

    def middle():
        await_arrivals(1, in_a, 4 * capacity)
        for part in range(wide_places // LANES):
            lanes = slice(part * LANES, (part + 1) * LANES)
            for c in range(3):
                points_m[c, :, lanes] = in_a[pl.ds(4 * LANES * part + c, LANES, stride=4), :].T
            coef_m0[:, lanes] = in_a[pl.ds(4 * LANES * part + 3, LANES, stride=4), :].T
            coef_m1[:, lanes] = answer[lanes, :].T
        advance(points_m, coef_m0, points_m, midway_m, 0.5 * time_step, 8)
        advance(midway_m, coef_m1, points_m, landed_m, time_step, 8)
        for part in range(wide_places // LANES):
            lanes = slice(part * LANES, (part + 1) * LANES)
            for c in range(3):
                tab_m[pl.ds(4 * LANES * part + c, LANES, stride=4), :] = landed_m[c, :, lanes].T
        turns.wait()
        place_rows(out_m, tab_m, turn_s, 0, 3)
        exchange(3, out_m, fin_m, 3 * capacity)

    middle()

    await_arrivals(2, answered, capacity)

    def fetch(g, carry):
        for s in range(8):
            b = g * 8 + s
            at = jnp.clip(index_s[2, b], 0, places - 1)
            tab_c[pl.ds(b, 1), :] = answered[pl.ds(at, 1), :]
        return carry

    lax.fori_loop(0, blocks // 8, fetch, 0)
    coef[...] = tab_c[...].T
    advance(midway, coef, start_points, landed, time_step, 16)

    group = 8

    def tabulate(g, sums):
        part = pl.ds(pl.multiple_of(g * group, group), group)
        lx = lagrange(landed[0, part, :])
        ly = lagrange(landed[1, part, :])
        lz = lagrange(landed[2, part, :])
        new = []
        for i in range(3):
            for j in range(3):
                xy = lx[i] * ly[j]
                for k in range(3):
                    value = xy * lz[k]
                    n = 9 * i + 3 * j + k
                    phi[n, part, :] = value
                    new.append(sums[n] + value * value)
        return tuple(new)

    zero = jnp.zeros((group, blocks), f32)
    squares = lax.fori_loop(0, markers // group, tabulate, (zero,) * 27)

    def moments(nodes):
        def gather(g, sums):
            for s in range(8):
                m = g * 8 + s
                values = carried[pl.ds(pl.multiple_of(m * fields, fields), fields), :]
                sums = tuple(
                    total + phi[n, pl.ds(m, 1), :] * values for total, n in zip(sums, nodes)
                )
            return sums

        zero = jnp.zeros((fields, blocks), f32)
        sums = lax.fori_loop(0, markers // 8, gather, (zero,) * len(nodes))
        for index, total in enumerate(sums):
            table[index * fields : (index + 1) * fields, :] = total

    per_row = LANES // fields
    full = 27 // per_row
    for j in range(2):
        moments(tuple(range(j * per_row, (j + 1) * per_row)))
        tab_e[pl.ds(j, blocks, stride=2), :] = table[...].T
    place_rows(out_e1, tab_e, index_s, 1, 2)
    exchange(4, out_e1, in_e1, 2 * capacity)

    moments(tuple(range(2 * per_row, 3 * per_row)))
    tab_e[pl.ds(0, blocks, stride=2), :] = table[...].T
    last = tuple(range(full * per_row, 27))
    moments(last)
    base = len(last) * fields
    table[base:LANES, :] = jnp.zeros((LANES - base, blocks), f32)
    for n in range(27):
        table[base + n : base + n + 1, :] = jnp.sum(squares[n], axis=0, keepdims=True)
    table[base + 27 : base + 28, :] = (elements[2:3, :] + 1).astype(f32)
    tab_e[pl.ds(1, blocks, stride=2), :] = table[...].T
    place_rows(out_e2, tab_e, index_s, 1, 2)
    exchange(5, out_e2, in_e2, 2 * capacity)

    for phase, arrived, onward, final in ((4, in_e1, on_e1, fin_e1), (5, in_e2, on_e2, fin_e2)):
        await_arrivals(phase, arrived, 2 * capacity)
        place_rows(onward, arrived, turn_s, 1, 2)
        exchange(phase + 2, onward, final, 2 * capacity)

    await_arrivals(3, fin_m, 3 * capacity)
    await_arrivals(6, fin_e1, 2 * capacity)
    await_arrivals(7, fin_e2, 2 * capacity)
    await_sends(0, request, 1)
    await_sends(1, out_a, 4 * capacity)
    await_sends(2, answer, capacity)
    await_sends(3, out_m, 3 * capacity)
    await_sends(4, out_e1, 2 * capacity)
    await_sends(5, out_e2, 2 * capacity)
    await_sends(6, on_e1, 2 * capacity)
    await_sends(7, on_e2, 2 * capacity)


def settle(fields, places, landed, first, second, moved, projected):
    owned = projected.shape[2]
    per_row = LANES // fields
    base = (27 - 27 // per_row * per_row) * fields
    for c in range(3):
        moved[c] = landed[pl.ds(c, places, stride=3), :]
    rows = [ref[pl.ds(j, places, stride=2), :] for ref in (first, second) for j in range(2)]
    full = 3
    element = rows[full][:, base + 27 : base + 28].astype(i32)
    hits = mask(iota((places, owned), 1) + 1 == element)

    def total(lines):
        high, low = split(lines.T)
        return dot(high, hits, ((1,), (0,))) + dot(low, hits, ((1,), (0,)))

    tail = total(rows[full])
    inverse = 1.0 / (1.0 + tail[base : base + 27, :])
    node = 0
    for j in range(full):
        sums = total(rows[j])
        for n in range(per_row):
            projected[node] = sums[n * fields : (n + 1) * fields, :] * inverse[node : node + 1, :]
            node += 1
    for n in range(27 - node):
        projected[node + n] = (
            tail[n * fields : (n + 1) * fields, :] * inverse[node + n : node + n + 1, :]
        )


def per_device(n_lat, n_rad, positions, fields, velocity, counts, elements, routes):
    blocks, _, markers = positions.shape
    n_fields = fields.shape[1]
    capacity = max(1, 2 * blocks // (3 * n_rad))
    slots = 3 * n_rad
    places = slots * capacity
    owned = velocity.shape[1]
    wide_places = round_up(places + 1, LANES)
    vmem = pl.BlockSpec(memory_space=pltpu.VMEM)
    anywhere = pl.BlockSpec(memory_space=pl.ANY)

    def rows(n):
        return pltpu.VMEM((round_up(n, 8), LANES), f32)

    small = pltpu.VMEM((slots, 2, LANES), f32)
    points = pltpu.VMEM((3, markers, blocks), f32)
    wide_points = pltpu.VMEM((3, markers, wide_places), f32)
    square = pltpu.VMEM((LANES, LANES), f32)
    pair = rows(2 * places)
    arrived = rows(2 * places + 2)
    index = pltpu.VMEM((8, wide_places), i32)
    index_s = pltpu.SMEM((8, wide_places), i32)
    final = pl.pallas_call(
        functools.partial(trip, n_lat, n_rad, capacity),
        out_shape=[jax.ShapeDtypeStruct((n * places, LANES), f32) for n in (3, 2, 2)],
        in_specs=[pl.BlockSpec(memory_space=pltpu.SMEM)] + [anywhere] * 5,
        out_specs=[vmem] * 3,
        scratch_shapes=[
            pltpu.VMEM((3, blocks, markers), f32),
            pltpu.VMEM(velocity.shape, f32),
            pltpu.VMEM(elements.shape, i32),
            pltpu.VMEM(routes.shape, i32),
            pltpu.VMEM(fields.shape, fields.dtype),
            rows(blocks * n_fields + n_fields),
            rows(markers * n_fields + n_fields),
            points, points, points,
            square,
            pltpu.VMEM((27, markers, blocks), f32),
            square,
            rows(4 * blocks + 4), rows(2 * blocks + 2), square,
            rows(4 * wide_places + 8),
            wide_points, wide_points, wide_points,
            pltpu.VMEM((LANES, wide_places), f32), pltpu.VMEM((LANES, wide_places), f32),
            small, small,
            rows(4 * places), rows(4 * wide_places + 8),
            rows(wide_places), rows(places), rows(3 * places),
            pair, arrived, pair, pair, arrived, pair,
            index, index, index_s, index_s,
            pltpu.SemaphoreType.DMA((8,)),
            pltpu.SemaphoreType.DMA((8,)),
            pltpu.SemaphoreType.DMA((8,)),
        ],
        compiler_params=pltpu.CompilerParams(collective_id=0, has_side_effects=True),
        name="trip",
    )(counts, jnp.transpose(positions, (1, 0, 2)), velocity, elements, routes, fields)
    moved, projected = pl.pallas_call(
        functools.partial(settle, n_fields, places),
        out_shape=(
            jax.ShapeDtypeStruct((3, places, markers), f32),
            jax.ShapeDtypeStruct((27, n_fields, owned), f32),
        ),
        in_specs=[vmem] * 3,
        out_specs=(vmem, vmem),
        name="settle",
    )(*final)
    return jnp.transpose(moved, (1, 0, 2)), projected


def solution(mesh):
    in_specs = (
        P(("lat", "rad"), None, None),
        P(("lat", "rad"), None, None),
        P(None, ("lat", "rad")),
        P(("lat", "rad")),
        P(None, ("lat", "rad")),
        P(None, ("lat", "rad")),
    )
    out_specs = (P(("lat", "rad"), None, None), P(None, None, ("lat", "rad")))
    return jax.shard_map(
        functools.partial(per_device, mesh.shape["lat"], mesh.shape["rad"]),
        mesh=mesh, in_specs=in_specs, out_specs=out_specs, check_vma=False,
    )
```

```python
import functools

import jax
import jax.numpy as jnp
from jax import lax
from jax.experimental import pallas as pl
from jax.experimental.pallas import tpu as pltpu
from jax.sharding import PartitionSpec as P

time_step = 0.4
MESH = pl.DeviceIdType.MESH
LANES = 128
bf16, f32, i32 = jnp.bfloat16, jnp.float32, jnp.int32


def round_up(x, by):
    return -(-x // by) * by


def split(x):
    high = x.astype(bf16)
    low = (x - high.astype(f32)).astype(bf16)
    return high, low


def dot(a, b, dims):
    return lax.dot_general(a, b, (dims, ((), ())), preferred_element_type=f32)


def iota(shape, axis):
    return lax.broadcasted_iota(i32, shape, axis)


def mask(condition):
    return condition.astype(f32).astype(bf16)


def lagrange(s):
    return (2.0 * (s - 0.5) * (s - 1.0), -4.0 * s * (s - 1.0), 2.0 * s * (s - 0.5))


def advance(points_in, coefficients, base, out, scale, group):
    markers = base.shape[1]

    def step(g, carry):
        rows = pl.ds(pl.multiple_of(g * group, group), group)
        lx = lagrange(points_in[0, rows, :])
        ly = lagrange(points_in[1, rows, :])
        lz = lagrange(points_in[2, rows, :])
        sums = [None] * 3
        for i in range(3):
            inner = [None] * 3
            for j in range(3):
                for c in range(3):
                    n = c * 27 + 9 * i + 3 * j
                    line = (
                        coefficients[n : n + 1, :] * lz[0]
                        + coefficients[n + 1 : n + 2, :] * lz[1]
                        + coefficients[n + 2 : n + 3, :] * lz[2]
                    ) * ly[j]
                    inner[c] = line if inner[c] is None else inner[c] + line
            for c in range(3):
                term = inner[c] * lx[i]
                sums[c] = term if sums[c] is None else sums[c] + term
        for c in range(3):
            out[c, rows, :] = base[c, rows, :] + scale * sums[c]
        return carry

    lax.fori_loop(0, markers // group, step, 0)


def parities(capacity):
    return ((0, 2), (1, 2)) if capacity % 2 == 0 else ((0, 1),)


def trip(
    n_lat, n_rad, capacity,
    counts, pos_in, vel_in, elements_in, routes_in, fld_in,
    fin_m, fin_t, fin_r, fin_e, weights,
    pos, vel, elements, routes, raw, wide, carried,
    start_points, midway, landed, coef, phi, table,
    tab_a1, tab_a2, tab_t, tab_r, tab_e, tab_c, tab_m, first_t, second_t,
    points_m, midway_m, landed_m, coef_m0, coef_m1,
    request, asked, out_a1, in_a1, out_a2, in_a2, answer, answered, out_m,
    out_t, in_t, on_t, out_r, in_r, on_r, out_e, in_e, on_e,
    index_v, turn_v, index_s, turn_s,
    load_sem, send_sem, recv_sem,
):
    lat, rad = lax.axis_index("lat"), lax.axis_index("rad")
    slots = 3 * n_rad
    places = slots * capacity
    shared = (capacity + 1) // 2
    blocks, fields, markers = fld_in.shape
    n_vel, owned = vel.shape
    wide_places = points_m.shape[2]

    def load(index, source, target):
        copy = pltpu.make_async_copy(source, target, load_sem.at[index])
        copy.start()
        return copy

    load_routes = load(0, routes_in, routes)
    load_elements = load(1, elements_in, elements)
    load_pos = load(2, pos_in, pos)
    load_vel = load(3, vel_in, vel)
    load_fld = load(4, fld_in, raw)

    def partner(k, q, back):
        by = (1 - k) if back else (k - 1)
        return lax.rem(lat + by + n_lat, n_lat), q

    barrier = pltpu.get_barrier_semaphore()
    for k in range(3):

        def greet(dq, carry, k=k):
            q = lax.rem(rad + dq, n_rad)
            pl.semaphore_signal(
                barrier, inc=1, device_id=partner(k, q, False), device_id_type=MESH
            )
            return carry

        lax.fori_loop(1 if k == 1 else 0, n_rad, greet, 0)

    def exchange(phase, source, target, size, back=False):
        for k in (0, 2, 1):

            def send(dq, carry, k=k):
                q = lax.rem(rad + dq, n_rad)
                pltpu.make_async_remote_copy(
                    src_ref=source.at[pl.ds((k * n_rad + q) * size, size)],
                    dst_ref=target.at[pl.ds((k * n_rad + rad) * size, size)],
                    send_sem=send_sem.at[phase],
                    recv_sem=recv_sem.at[phase],
                    device_id=partner(k, q, back),
                    device_id_type=MESH,
                ).start()
                return carry

            lax.fori_loop(1 if k == 1 else 0, n_rad, send, 0)
        own = pl.ds((n_rad + rad) * size, size)
        pltpu.make_async_copy(source.at[own], target.at[own], recv_sem.at[phase]).start()

    def await_arrivals(phase, target, size):
        part = target.at[pl.ds(0, slots * size)]
        pltpu.make_async_copy(part, part, recv_sem.at[phase]).wait()

    def await_sends(phase, source, size):
        part = source.at[pl.ds(0, (slots - 1) * size)]
        pltpu.make_async_copy(part, part, send_sem.at[phase]).wait()

    def slot_of(place):
        return jnp.floor((place.astype(f32) + 0.5) * (1.0 / capacity)).astype(i32)

    def within(source, at, rows):
        bits = (source.shape[0] - rows + 1).bit_length() - 1
        return at & ((1 << bits) - 1)

    def place_rows(out, source, indices, row, rows):
        def one(s, carry):
            for c in range(capacity):
                p = s * capacity + c
                at = within(source, indices[row, p], rows)
                out[pl.ds(p * rows, rows), :] = source[pl.ds(at, rows), :]
            return carry

        lax.fori_loop(0, slots, one, 0)

    def place_tails(out, sources, indices):
        lower = iota((1, LANES), 1) < LANES // 2

        def one(s, carry):
            for pair in range(shared):
                halves = []
                for half, source in enumerate(sources):
                    p = s * capacity + jnp.minimum(2 * pair + half, capacity - 1)
                    at = within(source, indices[1, p], 1)
                    halves.append(source[pl.ds(at, 1), :])
                line = jnp.where(lower, halves[0], halves[1])
                out[pl.ds(s * shared + pair, 1), :] = line
            return carry

        lax.fori_loop(0, slots, one, 0)

    def clear(ref, start):
        ref[start:, :] = jnp.zeros((ref.shape[0] - start, LANES), f32)

    for ref, start in (
        (tab_a1, 2 * blocks), (tab_a2, 2 * blocks), (tab_t, blocks), (tab_r, blocks),
        (tab_e, 2 * blocks), (in_a1, 2 * places), (in_a2, 2 * places), (first_t, places),
        (second_t, places), (in_r, places), (in_e, 2 * places), (answer, 0), (coef, 0),
    ):
        clear(ref, start)
    index_v[...] = jnp.zeros(index_v.shape, i32)
    turn_v[...] = jnp.zeros(turn_v.shape, i32)

    load_routes.wait()
    load_elements.wait()
    route = jnp.where(iota((1, blocks), 1) < counts[0], routes[0:1, :], -1)
    slot = slot_of(route)
    sent_to = iota((slots, blocks), 0) == slot
    inside = mask(iota((LANES, blocks), 0) == route - slot * capacity)
    for row, label in enumerate((elements[1:2, :], routes[1:2, :])):
        marked = jnp.where(sent_to, (label + 1).astype(f32), 0.0).astype(bf16)
        request[:, row, :] = dot(marked, inside, ((1,), (1,)))
    spread = mask(iota((index_v.shape[1], blocks), 0) == route)
    numbers = (iota((8, blocks), 1) - blocks).astype(f32).astype(bf16)
    holder = (dot(numbers, spread, ((1,), (1,))) + float(blocks)).astype(i32)
    index_v[0:1, :] = holder[0:1, :] * 2
    index_v[1:2, :] = holder[0:1, :]
    index_v[2:3, 0:blocks] = jnp.maximum(route, 0)
    indices = load(5, index_v, index_s)
    load_pos.wait()
    for c in range(2):
        tab_a1[pl.ds(c, blocks, stride=2), :] = pos[c]
    tab_a2[pl.ds(0, blocks, stride=2), :] = pos[2]
    indices.wait()
    place_rows(out_a1, tab_a1, index_s, 0, 2)
    pl.semaphore_wait(barrier, slots - 1)
    exchange(0, request, asked, 1)
    exchange(1, out_a1, in_a1, 2 * capacity)

    load_vel.wait()
    vel_high, vel_low = split(vel[...])
    pick = mask(iota((owned, blocks), 0) == elements[0:1, :])
    coef[0:n_vel, :] = dot(vel_high, pick, ((1,), (0,))) + dot(vel_low, pick, ((1,), (0,)))
    tab_a2[pl.ds(1, blocks, stride=2), :] = coef[...].T
    place_rows(out_a2, tab_a2, index_s, 0, 2)

    for c in range(3):
        start_points[c] = pos[c].T
    advance(start_points, coef, start_points, midway, 0.5 * time_step, 16)

    own_slot = slot_of(iota((places, slots), 0))
    by_slot = mask(own_slot == iota((places, slots), 1))
    lane = iota((places, LANES), 0) - slot_of(iota((places, LANES), 0)) * capacity
    by_lane = lane == iota((places, LANES), 1)

    def label_column(row):
        lines = dot(by_slot, asked[:, row, :].astype(bf16), ((1,), (0,)))
        return jnp.sum(jnp.where(by_lane, lines, 0.0), axis=1, keepdims=True).astype(i32)

    await_arrivals(0, asked, 1)
    pick = mask(iota((places, owned), 1) + 1 == label_column(0))
    answer[0:places, 0:n_vel] = dot(pick, vel_high, ((1,), (1,))) + dot(
        pick, vel_low, ((1,), (1,))
    )
    exchange(2, answer, answered, capacity, back=True)
    exchange(3, out_a2, in_a2, 2 * capacity)

    turned = mask(iota((places, turn_v.shape[1]), 1) + 1 == label_column(1))
    numbers = (iota((8, places), 1) - places).astype(f32).astype(bf16)
    holder = (dot(numbers, turned, ((1,), (0,))) + float(places)).astype(i32)
    turn_v[0:1, :] = holder[0:1, :] * 4
    turn_v[1:2, :] = holder[0:1, :]
    turn_v[2:3, :] = holder[0:1, :] * 2
    turns = load(6, turn_v, turn_s)
    load_fld.wait()
    wide[0 : blocks * fields, :] = raw[...].astype(f32).reshape(blocks * fields, markers)
    for f in range(fields):
        carried[pl.ds(f, markers, stride=fields), :] = wide[pl.ds(f, blocks, stride=fields), :].T

    await_arrivals(2, answered, capacity)

    def fetch(g, carry):
        for s in range(8):
            b = g * 8 + s
            at = within(answered, index_s[2, b], 1)
            tab_c[pl.ds(b, 1), :] = answered[pl.ds(at, 1), :]
        return carry

    lax.fori_loop(0, blocks // 8, fetch, 0)
    coef[...] = tab_c[...].T
    advance(midway, coef, start_points, landed, time_step, 16)

    group = 8

    def basis(points, part, lanes):
        lx = lagrange(points[0, part, lanes])
        ly = lagrange(points[1, part, lanes])
        lz = lagrange(points[2, part, lanes])
        for i in range(3):
            for j in range(3):
                xy = lx[i] * ly[j]
                for k in range(3):
                    yield 9 * i + 3 * j + k, xy * lz[k]

    def tabulate(g, carry):
        part = pl.ds(pl.multiple_of(g * group, group), group)
        for n, value in basis(landed, part, slice(0, blocks)):
            phi[n, part, :] = value
        return carry

    lax.fori_loop(0, markers // group, tabulate, 0)

    def moments(nodes):
        def gather(g, sums):
            for s in range(8):
                m = g * 8 + s
                values = carried[pl.ds(pl.multiple_of(m * fields, fields), fields), :]
                sums = tuple(
                    total + phi[n, pl.ds(m, 1), :] * values for total, n in zip(sums, nodes)
                )
            return sums

        zero = jnp.zeros((fields, blocks), f32)
        sums = lax.fori_loop(0, markers // 8, gather, (zero,) * len(nodes))
        for index, total in enumerate(sums):
            table[index * fields : (index + 1) * fields, :] = total

    per_row = LANES // fields
    full = 27 // per_row
    last = tuple(range(full * per_row, 27))
    base = len(last) * fields
    half = LANES // 2
    moments(last)
    table[base:half, :] = jnp.zeros((half - base, blocks), f32)
    table[base : base + 1, :] = (elements[2:3, :] + 1).astype(f32)
    table[half:, :] = table[0:half, :]
    tab_t[0:blocks, :] = table[...].T
    place_tails(out_t, (tab_t, tab_t), index_s)
    exchange(4, out_t, in_t, shared)
    moments(tuple(range(per_row)))
    tab_r[0:blocks, :] = table[...].T
    place_rows(out_r, tab_r, index_s, 1, 1)
    exchange(5, out_r, in_r, capacity)

    for j in range(2):
        moments(tuple(range((j + 1) * per_row, (j + 2) * per_row)))
        tab_e[pl.ds(j, blocks, stride=2), :] = table[...].T
    place_rows(out_e, tab_e, index_s, 0, 2)
    exchange(6, out_e, in_e, 2 * capacity)

    await_arrivals(1, in_a1, 2 * capacity)
    await_arrivals(3, in_a2, 2 * capacity)
    for part in range(wide_places // LANES):
        lanes = slice(part * LANES, (part + 1) * LANES)
        for c, (ref, row) in enumerate(((in_a1, 0), (in_a1, 1), (in_a2, 0))):
            points_m[c, :, lanes] = ref[pl.ds(2 * LANES * part + row, LANES, stride=2), :].T
        coef_m0[:, lanes] = in_a2[pl.ds(2 * LANES * part + 1, LANES, stride=2), :].T
        coef_m1[:, lanes] = answer[lanes, :].T
    advance(points_m, coef_m0, points_m, midway_m, 0.5 * time_step, 8)
    advance(midway_m, coef_m1, points_m, landed_m, time_step, 8)
    for part in range(wide_places // LANES):
        lanes = slice(part * LANES, (part + 1) * LANES)
        for c in range(3):
            tab_m[pl.ds(4 * LANES * part + c, LANES, stride=4), :] = landed_m[c, :, lanes].T
    turns.wait()
    place_rows(out_m, tab_m, turn_s, 0, 3)
    exchange(7, out_m, fin_m, 3 * capacity)

    await_arrivals(4, in_t, shared)
    tails = in_t[...]
    swapped = pltpu.roll(tails, half, 1)
    count = slots * shared
    for start, stride in parities(capacity):
        first_t[pl.ds(start, count, stride=stride), :] = swapped if start else tails
        second_t[pl.ds(start, count, stride=stride), :] = tails if start else swapped
    place_tails(on_t, (first_t, second_t), turn_s)
    exchange(8, on_t, fin_t, shared)
    await_arrivals(5, in_r, capacity)
    place_rows(on_r, in_r, turn_s, 1, 1)
    exchange(9, on_r, fin_r, capacity)
    await_arrivals(6, in_e, 2 * capacity)
    place_rows(on_e, in_e, turn_s, 2, 2)
    exchange(10, on_e, fin_e, 2 * capacity)

    await_arrivals(7, fin_m, 3 * capacity)
    halves = parities(capacity)
    count = places // len(halves)
    lanes_each = weights.shape[1] // len(halves)
    for index, (start, stride) in enumerate(halves):
        for c in range(3):
            tab_m[0:count, :] = fin_m[pl.ds(3 * start + c, count, stride=3 * stride), :]
            for part in range(lanes_each // LANES):
                at = index * lanes_each + part * LANES
                points_m[c, :, at : at + LANES] = tab_m[part * LANES : (part + 1) * LANES, :].T
    for part in range(weights.shape[1] // LANES):
        lanes = slice(part * LANES, (part + 1) * LANES)

        def square(g, sums, lanes=lanes):
            part = pl.ds(pl.multiple_of(g * group, group), group)
            return tuple(sums[n] + value * value for n, value in basis(points_m, part, lanes))

        zero = jnp.zeros((group, LANES), f32)
        sums = lax.fori_loop(0, markers // group, square, (zero,) * 27)
        for n in range(27):
            weights[n : n + 1, lanes] = jnp.sum(sums[n], axis=0, keepdims=True)
        weights[27:, lanes] = jnp.zeros((weights.shape[0] - 27, LANES), f32)

    await_arrivals(8, fin_t, shared)
    await_arrivals(9, fin_r, capacity)
    await_arrivals(10, fin_e, 2 * capacity)
    await_sends(0, request, 1)
    await_sends(1, out_a1, 2 * capacity)
    await_sends(2, answer, capacity)
    await_sends(3, out_a2, 2 * capacity)
    await_sends(4, out_t, shared)
    await_sends(5, out_r, capacity)
    await_sends(6, out_e, 2 * capacity)
    await_sends(7, out_m, 3 * capacity)
    await_sends(8, on_t, shared)
    await_sends(9, on_r, capacity)
    await_sends(10, on_e, 2 * capacity)


def settle(fields, capacity, landed, tails, first, rest, weights, moved, projected):
    owned = projected.shape[2]
    places = landed.shape[0] // 3
    per_row = LANES // fields
    full = 27 // per_row
    base = (27 - full * per_row) * fields
    half = LANES // 2
    for c in range(3):
        moved[c] = landed[pl.ds(c, places, stride=3), :]
    halves = parities(capacity)
    count = places // len(halves)
    lanes_each = weights.shape[1] // len(halves)
    hits = []
    for index in range(len(halves)):
        at = index * half + base
        element = tails[:, at : at + 1].astype(i32)
        hits.append(mask(iota((count, owned), 1) + 1 == element))

    def total(lines, index):
        high, low = split(lines)
        return dot(high, hits[index], ((1,), (0,))) + dot(low, hits[index], ((1,), (0,)))

    def summed(lines):
        return functools.reduce(jnp.add, [total(l, index) for index, l in enumerate(lines)])

    lanes = [slice(index * lanes_each, index * lanes_each + count) for index in range(len(halves))]
    inverse = 1.0 / (1.0 + summed([weights[:, l] for l in lanes]))
    turned = tails[...].T
    ends = summed([turned[index * half : (index + 1) * half] for index in range(len(halves))])
    node = 0
    for j in range(full):
        ref, row, rows = ((first, 0, 1), (rest, 0, 2), (rest, 1, 2))[j]
        sums = summed(
            [ref[pl.ds(rows * start + row, count, stride=rows * stride), :].T
             for start, stride in halves]
        )
        for n in range(per_row):
            projected[node] = sums[n * fields : (n + 1) * fields, :] * inverse[node : node + 1, :]
            node += 1
    for n in range(27 - node):
        projected[node + n] = (
            ends[n * fields : (n + 1) * fields, :] * inverse[node + n : node + n + 1, :]
        )


def per_device(n_lat, n_rad, positions, fields, velocity, counts, elements, routes):
    blocks, _, markers = positions.shape
    n_fields = fields.shape[1]
    capacity = max(1, 2 * blocks // (3 * n_rad))
    slots = 3 * n_rad
    places = slots * capacity
    shared = slots * ((capacity + 1) // 2)
    owned = velocity.shape[1]
    wide_places = round_up(places + 1, LANES)
    halves = len(parities(capacity))
    weight_lanes = halves * round_up(places // halves, LANES)
    vmem = pl.BlockSpec(memory_space=pltpu.VMEM)
    anywhere = pl.BlockSpec(memory_space=pltpu.HBM)

    def rows(n):
        return pltpu.VMEM((round_up(n, 8), LANES), f32)

    def looked_up(n, each):
        return rows((1 << (n * each).bit_length()) + each)

    small = pltpu.VMEM((slots, 2, LANES), f32)
    points = pltpu.VMEM((3, markers, blocks), f32)
    wide_points = pltpu.VMEM((3, markers, wide_places), f32)
    square = pltpu.VMEM((LANES, LANES), f32)
    index = pltpu.VMEM((8, wide_places), i32)
    index_s = pltpu.SMEM((8, wide_places), i32)
    final_rows = (3 * places, shared, places, 2 * places)
    inputs = (jnp.transpose(positions, (1, 0, 2)), velocity, elements, routes, fields)
    final = pl.pallas_call(
        functools.partial(trip, n_lat, n_rad, capacity),
        out_shape=[jax.ShapeDtypeStruct((n, LANES), f32) for n in final_rows]
        + [jax.ShapeDtypeStruct((32, weight_lanes), f32)],
        in_specs=[pl.BlockSpec(memory_space=pltpu.SMEM)] + [anywhere] * 5,
        out_specs=[vmem] * 5,
        scratch_shapes=[
            pltpu.VMEM((3, blocks, markers), f32),
            pltpu.VMEM(velocity.shape, f32),
            pltpu.VMEM(elements.shape, i32),
            pltpu.VMEM(routes.shape, i32),
            pltpu.VMEM(fields.shape, fields.dtype),
            rows((blocks + 1) * n_fields), rows((markers + 1) * n_fields),
            points, points, points,
            square,
            pltpu.VMEM((27, markers, blocks), f32),
            square,
            looked_up(blocks, 2), looked_up(blocks, 2),
            looked_up(blocks, 1), looked_up(blocks, 1), looked_up(blocks, 2),
            square, looked_up(wide_places - 1, 4),
            looked_up(places, 1), looked_up(places, 1),
            wide_points, wide_points, wide_points,
            pltpu.VMEM((LANES, wide_places), f32), pltpu.VMEM((LANES, wide_places), f32),
            small, small,
            rows(2 * places), rows(2 * wide_places + 8),
            rows(2 * places), rows(2 * wide_places + 8),
            rows(wide_places), looked_up(places, 1), rows(3 * places),
            rows(shared), rows(shared), rows(shared),
            rows(places), looked_up(places, 1), rows(places),
            rows(2 * places), looked_up(places, 2), rows(2 * places),
            index, index, index_s, index_s,
            pltpu.SemaphoreType.DMA((8,)),
            pltpu.SemaphoreType.DMA((11,)),
            pltpu.SemaphoreType.DMA((11,)),
        ],
        compiler_params=pltpu.CompilerParams(
            collective_id=0, has_side_effects=True, vmem_limit_bytes=24 * 1024 * 1024
        ),
        name="trip",
    )(counts, *[pltpu.with_memory_space_constraint(x, pltpu.HBM) for x in inputs])
    moved, projected = pl.pallas_call(
        functools.partial(settle, n_fields, capacity),
        out_shape=(
            jax.ShapeDtypeStruct((3, places, markers), f32),
            jax.ShapeDtypeStruct((27, n_fields, owned), f32),
        ),
        in_specs=[vmem] * 5,
        out_specs=(vmem, vmem),
        compiler_params=pltpu.CompilerParams(vmem_limit_bytes=16 * 1024 * 1024),
        name="settle",
    )(*final)
    return jnp.transpose(moved, (1, 0, 2)), projected


def solution(mesh):
    in_specs = (
        P(("lat", "rad"), None, None),
        P(("lat", "rad"), None, None),
        P(None, ("lat", "rad")),
        P(("lat", "rad")),
        P(None, ("lat", "rad")),
        P(None, ("lat", "rad")),
    )
    out_specs = (P(("lat", "rad"), None, None), P(None, None, ("lat", "rad")))
    return jax.shard_map(
        functools.partial(per_device, mesh.shape["lat"], mesh.shape["rad"]),
        mesh=mesh, in_specs=in_specs, out_specs=out_specs, check_vma=False,
    )
```

```python
import functools
import itertools

import jax
import jax.numpy as jnp
from jax import lax
from jax.experimental import pallas as pl
from jax.experimental.pallas import tpu as pltpu
from jax.sharding import PartitionSpec as P

time_step = 0.4
MESH = pl.DeviceIdType.MESH
LANES = 128
bf16, f32, i32 = jnp.bfloat16, jnp.float32, jnp.int32


def round_up(x, by):
    return -(-x // by) * by


def split(x):
    high = x.astype(bf16)
    low = (x - high.astype(f32)).astype(bf16)
    return high, low


def dot(a, b, dims):
    return lax.dot_general(a, b, (dims, ((), ())), preferred_element_type=f32)


def iota(shape, axis):
    return lax.broadcasted_iota(i32, shape, axis)


def mask(condition):
    return condition.astype(f32).astype(bf16)


def lagrange(s):
    return (2.0 * (s - 0.5) * (s - 1.0), -4.0 * s * (s - 1.0), 2.0 * s * (s - 0.5))


def advance(points_in, coefficients, base, out, scale, group):
    markers = base.shape[1]

    def step(g, carry):
        rows = pl.ds(pl.multiple_of(g * group, group), group)
        lx = lagrange(points_in[0, rows, :])
        ly = lagrange(points_in[1, rows, :])
        lz = lagrange(points_in[2, rows, :])
        sums = [None] * 3
        for i in range(3):
            inner = [None] * 3
            for j in range(3):
                for c in range(3):
                    n = c * 27 + 9 * i + 3 * j
                    line = (
                        coefficients[n : n + 1, :] * lz[0]
                        + coefficients[n + 1 : n + 2, :] * lz[1]
                        + coefficients[n + 2 : n + 3, :] * lz[2]
                    ) * ly[j]
                    inner[c] = line if inner[c] is None else inner[c] + line
            for c in range(3):
                term = inner[c] * lx[i]
                sums[c] = term if sums[c] is None else sums[c] + term
        for c in range(3):
            out[c, rows, :] = base[c, rows, :] + scale * sums[c]
        return carry

    lax.fori_loop(0, markers // group, step, 0)


def parities(capacity):
    return ((0, 2), (1, 2)) if capacity % 2 == 0 else ((0, 1),)


def trip(
    n_lat, n_rad, capacity,
    counts, pos_in, vel_in, elements_in, routes_in, fld_in,
    fin_m, fin_t, fin_r, fin_e, weights,
    pos, vel, elements, routes, raw, wide, carried,
    start_points, midway, landed, coef, phi, table,
    tab_a1, tab_a2, tab_t, tab_r, tab_e, tab_c, tab_m, first_t, second_t,
    points_m, midway_m, landed_m, coef_m0, coef_m1,
    request, asked, out_a1, in_a1, out_a2, in_a2, answer, answered, out_m,
    out_t, in_t, on_t, out_r, in_r, on_r, out_e, in_e, on_e,
    index_v, turn_v, index_s, turn_s,
    load_sem, send_sem, recv_sem,
):
    lat, rad = lax.axis_index("lat"), lax.axis_index("rad")
    slots = 3 * n_rad
    places = slots * capacity
    shared = (capacity + 1) // 2
    together = max(n for n in range(1, 5) if slots % n == 0)
    groups = round_up(slots // together, 8)
    blocks, fields, markers = fld_in.shape
    n_vel, owned = vel.shape
    wide_places = points_m.shape[2]

    def load(index, source, target):
        copy = pltpu.make_async_copy(source, target, load_sem.at[index])
        copy.start()
        return copy

    load_routes = load(0, routes_in, routes)
    load_elements = load(1, elements_in, elements)
    load_pos = load(2, pos_in, pos)
    load_vel = load(3, vel_in, vel)
    load_fld = load(4, fld_in, raw)

    def partner(k, q, back):
        by = (1 - k) if back else (k - 1)
        return lax.rem(lat + by + n_lat, n_lat), q

    barrier = pltpu.get_barrier_semaphore()
    for k in range(3):

        def greet(dq, carry, k=k):
            q = lax.rem(rad + dq, n_rad)
            pl.semaphore_signal(
                barrier, inc=1, device_id=partner(k, q, False), device_id_type=MESH
            )
            return carry

        lax.fori_loop(1 if k == 1 else 0, n_rad, greet, 0)

    def exchange(phase, source, target, size, back=False):
        for k in (0, 2, 1):

            def send(dq, carry, k=k):
                q = lax.rem(rad + dq, n_rad)
                pltpu.make_async_remote_copy(
                    src_ref=source.at[pl.ds((k * n_rad + q) * size, size)],
                    dst_ref=target.at[pl.ds((k * n_rad + rad) * size, size)],
                    send_sem=send_sem.at[phase],
                    recv_sem=recv_sem.at[phase],
                    device_id=partner(k, q, back),
                    device_id_type=MESH,
                ).start()
                return carry

            lax.fori_loop(1 if k == 1 else 0, n_rad, send, 0)
        own = pl.ds((n_rad + rad) * size, size)
        pltpu.make_async_copy(source.at[own], target.at[own], recv_sem.at[phase]).start()

    def await_arrivals(phase, target, size):
        part = target.at[pl.ds(0, slots * size)]
        pltpu.make_async_copy(part, part, recv_sem.at[phase]).wait()

    def await_sends(phase, source, size):
        part = source.at[pl.ds(0, (slots - 1) * size)]
        pltpu.make_async_copy(part, part, send_sem.at[phase]).wait()

    def slot_of(place, each=capacity):
        return jnp.floor((place.astype(f32) + 0.5) * (1.0 / each)).astype(i32)

    def grouped(place):
        group = slot_of(place, capacity * together)
        return group, place - group * (capacity * together)

    def within(source, at, rows):
        bits = (source.shape[0] - rows + 1).bit_length() - 1
        return at & ((1 << bits) - 1)

    def place_rows(out, source, indices, row, rows):
        at_once = capacity * together

        def some(g, carry):
            for c in range(at_once):
                p = g * at_once + c
                at = within(source, indices[row * groups + g, c], rows)
                out[pl.ds(p * rows, rows), :] = source[pl.ds(at, rows), :]
            return carry

        lax.fori_loop(0, slots // together, some, 0)

    def place_tails(out, sources, indices):
        lower = iota((1, LANES), 1) < LANES // 2

        def some(g, carry):
            for s, pair in itertools.product(range(together), range(shared)):
                halves = []
                for half, source in enumerate(sources):
                    c = s * capacity + min(2 * pair + half, capacity - 1)
                    at = within(source, indices[g, c], 1)
                    halves.append(source[pl.ds(at, 1), :])
                line = jnp.where(lower, halves[0], halves[1])
                out[pl.ds((g * together + s) * shared + pair, 1), :] = line
            return carry

        lax.fori_loop(0, slots // together, some, 0)

    def clear(ref, start):
        ref[start:, :] = jnp.zeros((ref.shape[0] - start, LANES), f32)

    for ref, start in (
        (tab_a1, 2 * blocks), (tab_a2, 2 * blocks), (tab_t, blocks), (tab_r, blocks),
        (tab_e, 2 * blocks), (in_a1, 2 * places), (in_a2, 2 * places), (first_t, places),
        (second_t, places), (in_r, places), (in_e, 2 * places), (answer, 0), (coef, 0),
    ):
        clear(ref, start)
    index_v[...] = jnp.zeros(index_v.shape, i32)
    turn_v[...] = jnp.zeros(turn_v.shape, i32)

    load_routes.wait()
    load_elements.wait()
    route = jnp.where(iota((1, blocks), 1) < counts[0], routes[0:1, :], -1)
    slot = slot_of(route)
    sent_to = iota((slots, blocks), 0) == slot
    inside = mask(iota((LANES, blocks), 0) == route - slot * capacity)
    for row, label in enumerate((elements[1:2, :], routes[1:2, :])):
        marked = jnp.where(sent_to, (label + 1).astype(f32), 0.0).astype(bf16)
        request[:, row, :] = dot(marked, inside, ((1,), (1,)))
    group_of, within_group = grouped(route)
    chosen = iota((groups, blocks), 0) == group_of
    numbers = iota((groups, blocks), 1) - blocks
    numbers = jnp.where(chosen, numbers.astype(f32), 0.0).astype(bf16)
    matched = mask(iota((LANES, blocks), 0) == within_group)
    holder = (dot(numbers, matched, ((1,), (1,))) + float(blocks)).astype(i32)
    for row in range(2):
        index_v[row * groups : (row + 1) * groups, :] = holder * (1 << row)
    index_v[2 * groups : 2 * groups + 1, 0:blocks] = jnp.maximum(route, 0)
    indices = load(5, index_v, index_s)
    load_pos.wait()
    for c in range(2):
        tab_a1[pl.ds(c, blocks, stride=2), :] = pos[c]
    tab_a2[pl.ds(0, blocks, stride=2), :] = pos[2]
    indices.wait()
    place_rows(out_a1, tab_a1, index_s, 1, 2)
    pl.semaphore_wait(barrier, slots - 1)
    exchange(0, request, asked, 1)
    exchange(1, out_a1, in_a1, 2 * capacity)

    load_vel.wait()
    vel_high, vel_low = split(vel[...])
    pick = mask(iota((owned, blocks), 0) == elements[0:1, :])
    coef[0:n_vel, :] = dot(vel_high, pick, ((1,), (0,))) + dot(vel_low, pick, ((1,), (0,)))
    tab_a2[pl.ds(1, blocks, stride=2), :] = coef[...].T
    place_rows(out_a2, tab_a2, index_s, 1, 2)

    for c in range(3):
        start_points[c] = pos[c].T
    advance(start_points, coef, start_points, midway, 0.5 * time_step, 16)

    own_slot = slot_of(iota((places, slots), 0))
    by_slot = mask(own_slot == iota((places, slots), 1))
    lane = iota((places, LANES), 0) - slot_of(iota((places, LANES), 0)) * capacity
    by_lane = lane == iota((places, LANES), 1)

    def label_column(row):
        lines = dot(by_slot, asked[:, row, :].astype(bf16), ((1,), (0,)))
        return jnp.sum(jnp.where(by_lane, lines, 0.0), axis=1, keepdims=True).astype(i32)

    await_arrivals(0, asked, 1)
    pick = mask(iota((places, owned), 1) + 1 == label_column(0))
    answer[0:places, 0:n_vel] = dot(pick, vel_high, ((1,), (1,))) + dot(
        pick, vel_low, ((1,), (1,))
    )
    exchange(2, answer, answered, capacity, back=True)
    exchange(3, out_a2, in_a2, 2 * capacity)

    group_of, within_group = grouped(label_column(1) - 1)
    chosen = iota((places, LANES), 1) == group_of
    numbers = iota((places, LANES), 0) - places
    numbers = jnp.where(chosen, numbers.astype(f32), 0.0).astype(bf16)
    matched = mask(iota((places, LANES), 1) == within_group)
    holder = (dot(numbers, matched, ((0,), (0,))) + float(places)).astype(i32)
    for row in range(3):
        turn_v[row * groups : (row + 1) * groups, :] = holder[0:groups, :] * (1 << row)
    turns = load(6, turn_v, turn_s)
    load_fld.wait()
    wide[0 : blocks * fields, :] = raw[...].astype(f32).reshape(blocks * fields, markers)
    for f in range(fields):
        carried[pl.ds(f, markers, stride=fields), :] = wide[pl.ds(f, blocks, stride=fields), :].T

    await_arrivals(2, answered, capacity)

    for b in range(blocks):
        at = within(answered, index_s[2 * groups, b], 1)
        tab_c[b : b + 1, :] = answered[pl.ds(at, 1), :]
    coef[...] = tab_c[...].T
    advance(midway, coef, start_points, landed, time_step, 16)

    group = 8

    def basis(points, part, lanes, only=range(27)):
        lx = lagrange(points[0, part, lanes])
        ly = lagrange(points[1, part, lanes])
        lz = lagrange(points[2, part, lanes])
        for i, j in itertools.product(range(3), range(3)):
            nodes = [n for n in range(9 * i + 3 * j, 9 * i + 3 * j + 3) if n in only]
            if nodes:
                xy = lx[i] * ly[j]
                for n in nodes:
                    yield n, xy * lz[n % 3]

    def tabulate(only, group):
        def some(g, carry):
            part = pl.ds(pl.multiple_of(g * group, group), group)
            for n, value in basis(landed, part, slice(0, blocks), only):
                phi[n, part, :] = value
            return carry

        lax.fori_loop(0, markers // group, some, 0)

    def moments(nodes):
        def gather(g, sums):
            for s in range(8):
                m = g * 8 + s
                values = carried[pl.ds(pl.multiple_of(m * fields, fields), fields), :]
                sums = tuple(
                    total + phi[n, pl.ds(m, 1), :] * values for total, n in zip(sums, nodes)
                )
            return sums

        zero = jnp.zeros((fields, blocks), f32)
        sums = lax.fori_loop(0, markers // 8, gather, (zero,) * len(nodes))
        for index, total in enumerate(sums):
            table[index * fields : (index + 1) * fields, :] = total

    per_row = LANES // fields
    full = 27 // per_row
    last = tuple(range(full * per_row, 27))
    base = len(last) * fields
    half = LANES // 2
    tabulate(last, 32)
    moments(last)
    table[base:half, :] = jnp.zeros((half - base, blocks), f32)
    table[base : base + 1, :] = (elements[2:3, :] + 1).astype(f32)
    table[half:, :] = table[0:half, :]
    tab_t[0:blocks, :] = table[...].T
    place_tails(out_t, (tab_t, tab_t), index_s)
    exchange(4, out_t, in_t, shared)
    tabulate(range(full * per_row), group)
    moments(tuple(range(per_row)))
    tab_r[0:blocks, :] = table[...].T
    place_rows(out_r, tab_r, index_s, 0, 1)
    exchange(5, out_r, in_r, capacity)

    for j in range(2):
        moments(tuple(range((j + 1) * per_row, (j + 2) * per_row)))
        tab_e[pl.ds(j, blocks, stride=2), :] = table[...].T
    place_rows(out_e, tab_e, index_s, 1, 2)
    exchange(6, out_e, in_e, 2 * capacity)

    await_arrivals(1, in_a1, 2 * capacity)
    await_arrivals(3, in_a2, 2 * capacity)
    for part in range(wide_places // LANES):
        lanes = slice(part * LANES, (part + 1) * LANES)
        for c, (ref, row) in enumerate(((in_a1, 0), (in_a1, 1), (in_a2, 0))):
            points_m[c, :, lanes] = ref[pl.ds(2 * LANES * part + row, LANES, stride=2), :].T
        coef_m0[:, lanes] = in_a2[pl.ds(2 * LANES * part + 1, LANES, stride=2), :].T
        coef_m1[:, lanes] = answer[lanes, :].T
    advance(points_m, coef_m0, points_m, midway_m, 0.5 * time_step, 8)
    advance(midway_m, coef_m1, points_m, landed_m, time_step, 8)
    for part in range(wide_places // LANES):
        lanes = slice(part * LANES, (part + 1) * LANES)
        for c in range(3):
            tab_m[pl.ds(4 * LANES * part + c, LANES, stride=4), :] = landed_m[c, :, lanes].T
    turns.wait()
    place_rows(out_m, tab_m, turn_s, 2, 3)
    exchange(7, out_m, fin_m, 3 * capacity)

    await_arrivals(4, in_t, shared)
    tails = in_t[...]
    swapped = pltpu.roll(tails, half, 1)
    count = slots * shared
    for start, stride in parities(capacity):
        first_t[pl.ds(start, count, stride=stride), :] = swapped if start else tails
        second_t[pl.ds(start, count, stride=stride), :] = tails if start else swapped
    place_tails(on_t, (first_t, second_t), turn_s)
    exchange(8, on_t, fin_t, shared)
    await_arrivals(5, in_r, capacity)
    place_rows(on_r, in_r, turn_s, 0, 1)
    exchange(9, on_r, fin_r, capacity)
    await_arrivals(6, in_e, 2 * capacity)
    place_rows(on_e, in_e, turn_s, 1, 2)
    exchange(10, on_e, fin_e, 2 * capacity)

    await_arrivals(7, fin_m, 3 * capacity)
    halves = parities(capacity)
    count = places // len(halves)
    lanes_each = weights.shape[1] // len(halves)
    for index, (start, stride) in enumerate(halves):
        for c in range(3):
            tab_m[0:count, :] = fin_m[pl.ds(3 * start + c, count, stride=3 * stride), :]
            for part in range(lanes_each // LANES):
                at = index * lanes_each + part * LANES
                points_m[c, :, at : at + LANES] = tab_m[part * LANES : (part + 1) * LANES, :].T
    for part in range(weights.shape[1] // LANES):
        lanes = slice(part * LANES, (part + 1) * LANES)

        def square(g, sums, lanes=lanes):
            part = pl.ds(pl.multiple_of(g * group, group), group)
            return tuple(sums[n] + value * value for n, value in basis(points_m, part, lanes))

        zero = jnp.zeros((group, LANES), f32)
        sums = lax.fori_loop(0, markers // group, square, (zero,) * 27)
        for n in range(27):
            weights[n : n + 1, lanes] = jnp.sum(sums[n], axis=0, keepdims=True)
        weights[27:, lanes] = jnp.zeros((weights.shape[0] - 27, LANES), f32)

    await_arrivals(8, fin_t, shared)
    await_arrivals(9, fin_r, capacity)
    await_arrivals(10, fin_e, 2 * capacity)
    await_sends(0, request, 1)
    await_sends(1, out_a1, 2 * capacity)
    await_sends(2, answer, capacity)
    await_sends(3, out_a2, 2 * capacity)
    await_sends(4, out_t, shared)
    await_sends(5, out_r, capacity)
    await_sends(6, out_e, 2 * capacity)
    await_sends(7, out_m, 3 * capacity)
    await_sends(8, on_t, shared)
    await_sends(9, on_r, capacity)
    await_sends(10, on_e, 2 * capacity)


def settle(fields, capacity, landed, tails, first, rest, weights, moved, projected):
    owned = projected.shape[2]
    places = landed.shape[0] // 3
    per_row = LANES // fields
    full = 27 // per_row
    base = (27 - full * per_row) * fields
    half = LANES // 2
    for c in range(3):
        moved[c] = landed[pl.ds(c, places, stride=3), :]
    halves = parities(capacity)
    count = places // len(halves)
    lanes_each = weights.shape[1] // len(halves)
    hits = []
    for index in range(len(halves)):
        at = index * half + base
        element = tails[:, at : at + 1].astype(i32)
        hits.append(mask(iota((count, owned), 1) + 1 == element))

    def total(lines, index):
        high, low = split(lines)
        return dot(high, hits[index], ((1,), (0,))) + dot(low, hits[index], ((1,), (0,)))

    def summed(lines):
        return functools.reduce(jnp.add, [total(l, index) for index, l in enumerate(lines)])

    lanes = [slice(index * lanes_each, index * lanes_each + count) for index in range(len(halves))]
    inverse = 1.0 / (1.0 + summed([weights[:, l] for l in lanes]))
    turned = tails[...].T
    ends = summed([turned[index * half : (index + 1) * half] for index in range(len(halves))])
    node = 0
    for j in range(full):
        ref, row, rows = ((first, 0, 1), (rest, 0, 2), (rest, 1, 2))[j]
        sums = summed(
            [ref[pl.ds(rows * start + row, count, stride=rows * stride), :].T
             for start, stride in halves]
        )
        for n in range(per_row):
            projected[node] = sums[n * fields : (n + 1) * fields, :] * inverse[node : node + 1, :]
            node += 1
    for n in range(27 - node):
        projected[node + n] = (
            ends[n * fields : (n + 1) * fields, :] * inverse[node + n : node + n + 1, :]
        )


def per_device(n_lat, n_rad, positions, fields, velocity, counts, elements, routes):
    blocks, _, markers = positions.shape
    n_fields = fields.shape[1]
    capacity = max(1, 2 * blocks // (3 * n_rad))
    slots = 3 * n_rad
    places = slots * capacity
    shared = slots * ((capacity + 1) // 2)
    owned = velocity.shape[1]
    wide_places = round_up(places + 1, LANES)
    halves = len(parities(capacity))
    weight_lanes = halves * round_up(places // halves, LANES)
    vmem = pl.BlockSpec(memory_space=pltpu.VMEM)
    anywhere = pl.BlockSpec(memory_space=pltpu.HBM)

    def rows(n):
        return pltpu.VMEM((round_up(n, 8), LANES), f32)

    def looked_up(n, each):
        return rows((1 << (n * each).bit_length()) + each)

    small = pltpu.VMEM((slots, 2, LANES), f32)
    points = pltpu.VMEM((3, markers, blocks), f32)
    wide_points = pltpu.VMEM((3, markers, wide_places), f32)
    square = pltpu.VMEM((LANES, LANES), f32)
    together = max(n for n in range(1, 5) if slots % n == 0)
    index_rows = 3 * round_up(slots // together, 8)
    index = pltpu.VMEM((index_rows, LANES), i32)
    index_s = pltpu.SMEM((index_rows, LANES), i32)
    final_rows = (3 * places, shared, places, 2 * places)
    inputs = (jnp.transpose(positions, (1, 0, 2)), velocity, elements, routes, fields)
    final = pl.pallas_call(
        functools.partial(trip, n_lat, n_rad, capacity),
        out_shape=[jax.ShapeDtypeStruct((n, LANES), f32) for n in final_rows]
        + [jax.ShapeDtypeStruct((32, weight_lanes), f32)],
        in_specs=[pl.BlockSpec(memory_space=pltpu.SMEM)] + [anywhere] * 5,
        out_specs=[vmem] * 5,
        scratch_shapes=[
            pltpu.VMEM((3, blocks, markers), f32),
            pltpu.VMEM(velocity.shape, f32),
            pltpu.VMEM(elements.shape, i32),
            pltpu.VMEM(routes.shape, i32),
            pltpu.VMEM(fields.shape, fields.dtype),
            rows((blocks + 1) * n_fields), rows((markers + 1) * n_fields),
            points, points, points,
            square,
            pltpu.VMEM((27, markers, blocks), f32),
            square,
            looked_up(blocks, 2), looked_up(blocks, 2),
            looked_up(blocks, 1), looked_up(blocks, 1), looked_up(blocks, 2),
            square, looked_up(wide_places - 1, 4),
            looked_up(places, 1), looked_up(places, 1),
            wide_points, wide_points, wide_points,
            pltpu.VMEM((LANES, wide_places), f32), pltpu.VMEM((LANES, wide_places), f32),
            small, small,
            rows(2 * places), rows(2 * wide_places + 8),
            rows(2 * places), rows(2 * wide_places + 8),
            rows(wide_places), looked_up(places, 1), rows(3 * places),
            rows(shared), rows(shared), rows(shared),
            rows(places), looked_up(places, 1), rows(places),
            rows(2 * places), looked_up(places, 2), rows(2 * places),
            index, index, index_s, index_s,
            pltpu.SemaphoreType.DMA((8,)),
            pltpu.SemaphoreType.DMA((11,)),
            pltpu.SemaphoreType.DMA((11,)),
        ],
        compiler_params=pltpu.CompilerParams(
            collective_id=0, has_side_effects=True, vmem_limit_bytes=24 * 1024 * 1024
        ),
        name="trip",
    )(counts, *[pltpu.with_memory_space_constraint(x, pltpu.HBM) for x in inputs])
    moved, projected = pl.pallas_call(
        functools.partial(settle, n_fields, capacity),
        out_shape=(
            jax.ShapeDtypeStruct((3, places, markers), f32),
            jax.ShapeDtypeStruct((27, n_fields, owned), f32),
        ),
        in_specs=[vmem] * 5,
        out_specs=(vmem, vmem),
        compiler_params=pltpu.CompilerParams(vmem_limit_bytes=16 * 1024 * 1024),
        name="settle",
    )(*final)
    return jnp.transpose(moved, (1, 0, 2)), projected


def solution(mesh):
    in_specs = (
        P(("lat", "rad"), None, None),
        P(("lat", "rad"), None, None),
        P(None, ("lat", "rad")),
        P(("lat", "rad")),
        P(None, ("lat", "rad")),
        P(None, ("lat", "rad")),
    )
    out_specs = (P(("lat", "rad"), None, None), P(None, None, ("lat", "rad")))
    return jax.shard_map(
        functools.partial(per_device, mesh.shape["lat"], mesh.shape["rad"]),
        mesh=mesh, in_specs=in_specs, out_specs=out_specs, check_vma=False,
    )
```

```python
import functools
import itertools

import jax
import jax.numpy as jnp
from jax import lax
from jax.experimental import pallas as pl
from jax.experimental.pallas import tpu as pltpu
from jax.sharding import PartitionSpec as P

time_step = 0.4
MESH = pl.DeviceIdType.MESH
LANES = 128
bf16, f32, i32 = jnp.bfloat16, jnp.float32, jnp.int32


def round_up(x, by):
    return -(-x // by) * by


def split(x):
    high = x.astype(bf16)
    low = (x - high.astype(f32)).astype(bf16)
    return high, low


def dot(a, b, dims):
    return lax.dot_general(a, b, (dims, ((), ())), preferred_element_type=f32)


def iota(shape, axis):
    return lax.broadcasted_iota(i32, shape, axis)


def mask(condition):
    return condition.astype(f32).astype(bf16)


def lagrange(s):
    return (2.0 * (s - 0.5) * (s - 1.0), -4.0 * s * (s - 1.0), 2.0 * s * (s - 0.5))


def advance(points_in, coefficients, base, out, scale, group):
    markers = base.shape[1]

    def step(g, carry):
        rows = pl.ds(pl.multiple_of(g * group, group), group)
        lx = lagrange(points_in[0, rows, :])
        ly = lagrange(points_in[1, rows, :])
        lz = lagrange(points_in[2, rows, :])
        sums = [None] * 3
        for i in range(3):
            inner = [None] * 3
            for j in range(3):
                for c in range(3):
                    n = c * 27 + 9 * i + 3 * j
                    line = (
                        coefficients[n : n + 1, :] * lz[0]
                        + coefficients[n + 1 : n + 2, :] * lz[1]
                        + coefficients[n + 2 : n + 3, :] * lz[2]
                    ) * ly[j]
                    inner[c] = line if inner[c] is None else inner[c] + line
            for c in range(3):
                term = inner[c] * lx[i]
                sums[c] = term if sums[c] is None else sums[c] + term
        for c in range(3):
            out[c, rows, :] = base[c, rows, :] + scale * sums[c]
        return carry

    lax.fori_loop(0, markers // group, step, 0)


def parities(capacity):
    return ((0, 2), (1, 2)) if capacity % 2 == 0 else ((0, 1),)


def trip(
    n_lat, n_rad, capacity,
    counts, pos_in, vel_in, elements_in, routes_in, fld_in,
    fin_m, fin_t, fin_r, fin_e, weights,
    pos, vel, elements, routes, raw, wide, carried,
    start_points, midway, landed, coef, phi, table,
    tab_a1, tab_a2, tab_t, tab_r, tab_e, tab_c, tab_m, first_t, second_t,
    points_m, midway_m, landed_m, coef_m0, coef_m1,
    request, asked, out_a1, in_a1, out_a2, in_a2, answer, answered, out_m,
    out_t, in_t, on_t, out_r, in_r, on_r, out_e, in_e, on_e,
    index_v, turn_v, index_s, turn_s,
    load_sem, send_sem, recv_sem,
):
    lat, rad = lax.axis_index("lat"), lax.axis_index("rad")
    slots = 3 * n_rad
    places = slots * capacity
    shared = (capacity + 1) // 2
    together = max(n for n in range(1, 5) if slots % n == 0)
    groups = round_up(slots // together, 8)
    blocks, fields, markers = fld_in.shape
    n_vel, owned = vel.shape
    wide_places = points_m.shape[2]

    def load(index, source, target):
        copy = pltpu.make_async_copy(source, target, load_sem.at[index])
        copy.start()
        return copy

    load_routes = load(0, routes_in, routes)
    load_elements = load(1, elements_in, elements)
    load_pos = load(2, pos_in, pos)
    load_vel = load(3, vel_in, vel)
    load_fld = load(4, fld_in, raw)

    def partner(k, q, back):
        by = (1 - k) if back else (k - 1)
        return lax.rem(lat + by + n_lat, n_lat), q

    def outward(back):
        first = 2 * (2 * lat // n_lat)
        return enumerate((2 - first, first, 1) if back else (first, 2 - first, 1))

    barrier = pltpu.get_barrier_semaphore()
    for place, k in outward(False):

        def greet(dq, carry, k=k):
            q = lax.rem(rad + dq, n_rad)
            pl.semaphore_signal(
                barrier, inc=1, device_id=partner(k, q, False), device_id_type=MESH
            )
            return carry

        lax.fori_loop(int(place == 2), n_rad, greet, 0)

    def exchange(phase, source, target, size, back=False):
        for place, k in outward(back):

            def send(dq, carry, k=k):
                q = lax.rem(rad + dq, n_rad)
                pltpu.make_async_remote_copy(
                    src_ref=source.at[pl.ds((k * n_rad + q) * size, size)],
                    dst_ref=target.at[pl.ds((k * n_rad + rad) * size, size)],
                    send_sem=send_sem.at[phase],
                    recv_sem=recv_sem.at[phase],
                    device_id=partner(k, q, back),
                    device_id_type=MESH,
                ).start()
                return carry

            lax.fori_loop(int(place == 2), n_rad, send, 0)
        own = pl.ds((n_rad + rad) * size, size)
        pltpu.make_async_copy(source.at[own], target.at[own], recv_sem.at[phase]).start()

    def await_arrivals(phase, target, size):
        part = target.at[pl.ds(0, slots * size)]
        pltpu.make_async_copy(part, part, recv_sem.at[phase]).wait()

    def await_sends(phase, source, size):
        part = source.at[pl.ds(0, (slots - 1) * size)]
        pltpu.make_async_copy(part, part, send_sem.at[phase]).wait()

    def slot_of(place, each=capacity):
        return jnp.floor((place.astype(f32) + 0.5) * (1.0 / each)).astype(i32)

    def grouped(place):
        group = slot_of(place, capacity * together)
        return group, place - group * (capacity * together)

    def within(source, at, rows):
        bits = (source.shape[0] - rows + 1).bit_length() - 1
        return at & ((1 << bits) - 1)

    def place_rows(out, source, indices, row, rows):
        at_once = capacity * together

        def some(g, carry):
            for c in range(at_once):
                p = g * at_once + c
                at = within(source, indices[row * groups + g, c], rows)
                out[pl.ds(p * rows, rows), :] = source[pl.ds(at, rows), :]
            return carry

        lax.fori_loop(0, slots // together, some, 0)

    def place_tails(out, sources, indices):
        lower = iota((1, LANES), 1) < LANES // 2

        def some(g, carry):
            for s, pair in itertools.product(range(together), range(shared)):
                halves = []
                for half, source in enumerate(sources):
                    c = s * capacity + min(2 * pair + half, capacity - 1)
                    at = within(source, indices[g, c], 1)
                    halves.append(source[pl.ds(at, 1), :])
                line = jnp.where(lower, halves[0], halves[1])
                out[pl.ds((g * together + s) * shared + pair, 1), :] = line
            return carry

        lax.fori_loop(0, slots // together, some, 0)

    def clear(ref, start):
        ref[start:, :] = jnp.zeros((ref.shape[0] - start, LANES), f32)

    for ref, start in (
        (tab_a1, 2 * blocks), (tab_a2, 2 * blocks), (tab_t, blocks), (tab_r, blocks),
        (tab_e, 2 * blocks), (in_a1, 2 * places), (in_a2, 2 * places), (first_t, places),
        (second_t, places), (in_r, places), (in_e, 2 * places), (answer, 0), (coef, 0),
    ):
        clear(ref, start)
    index_v[...] = jnp.zeros(index_v.shape, i32)
    turn_v[...] = jnp.zeros(turn_v.shape, i32)

    load_routes.wait()
    load_elements.wait()
    route = jnp.where(iota((1, blocks), 1) < counts[0], routes[0:1, :], -1)
    slot = slot_of(route)
    sent_to = iota((slots, blocks), 0) == slot
    inside = mask(iota((LANES, blocks), 0) == route - slot * capacity)
    for row, label in enumerate((elements[1:2, :], routes[1:2, :])):
        marked = jnp.where(sent_to, (label + 1).astype(f32), 0.0).astype(bf16)
        request[:, row, :] = dot(marked, inside, ((1,), (1,)))
    group_of, within_group = grouped(route)
    chosen = iota((groups, blocks), 0) == group_of
    numbers = iota((groups, blocks), 1) - blocks
    numbers = jnp.where(chosen, numbers.astype(f32), 0.0).astype(bf16)
    matched = mask(iota((LANES, blocks), 0) == within_group)
    holder = (dot(numbers, matched, ((1,), (1,))) + float(blocks)).astype(i32)
    for row in range(2):
        index_v[row * groups : (row + 1) * groups, :] = holder * (1 << row)
    index_v[2 * groups : 2 * groups + 1, 0:blocks] = jnp.maximum(route, 0)
    indices = load(5, index_v, index_s)
    load_pos.wait()
    for c in range(2):
        tab_a1[pl.ds(c, blocks, stride=2), :] = pos[c]
    tab_a2[pl.ds(0, blocks, stride=2), :] = pos[2]
    indices.wait()
    place_rows(out_a1, tab_a1, index_s, 1, 2)
    pl.semaphore_wait(barrier, slots - 1)
    exchange(0, request, asked, 1)
    exchange(1, out_a1, in_a1, 2 * capacity)

    load_vel.wait()
    vel_high, vel_low = split(vel[...])
    pick = mask(iota((owned, blocks), 0) == elements[0:1, :])
    coef[0:n_vel, :] = dot(vel_high, pick, ((1,), (0,))) + dot(vel_low, pick, ((1,), (0,)))
    tab_a2[pl.ds(1, blocks, stride=2), :] = coef[...].T
    place_rows(out_a2, tab_a2, index_s, 1, 2)

    for c in range(3):
        start_points[c] = pos[c].T
    advance(start_points, coef, start_points, midway, 0.5 * time_step, 16)

    own_slot = slot_of(iota((places, slots), 0))
    by_slot = mask(own_slot == iota((places, slots), 1))
    lane = iota((places, LANES), 0) - slot_of(iota((places, LANES), 0)) * capacity
    by_lane = lane == iota((places, LANES), 1)

    def label_column(row):
        lines = dot(by_slot, asked[:, row, :].astype(bf16), ((1,), (0,)))
        return jnp.sum(jnp.where(by_lane, lines, 0.0), axis=1, keepdims=True).astype(i32)

    await_arrivals(0, asked, 1)
    pick = mask(iota((places, owned), 1) + 1 == label_column(0))
    answer[0:places, 0:n_vel] = dot(pick, vel_high, ((1,), (1,))) + dot(
        pick, vel_low, ((1,), (1,))
    )
    exchange(2, answer, answered, capacity, back=True)

    group_of, within_group = grouped(label_column(1) - 1)
    chosen = iota((places, LANES), 1) == group_of
    numbers = iota((places, LANES), 0) - places
    numbers = jnp.where(chosen, numbers.astype(f32), 0.0).astype(bf16)
    matched = mask(iota((places, LANES), 1) == within_group)
    holder = (dot(numbers, matched, ((0,), (0,))) + float(places)).astype(i32)
    for row in range(3):
        turn_v[row * groups : (row + 1) * groups, :] = holder[0:groups, :] * (1 << row)
    turns = load(6, turn_v, turn_s)
    load_fld.wait()
    wide[0 : blocks * fields, :] = raw[...].astype(f32).reshape(blocks * fields, markers)
    for f in range(fields):
        carried[pl.ds(f, markers, stride=fields), :] = wide[pl.ds(f, blocks, stride=fields), :].T

    exchange(3, out_a2, in_a2, 2 * capacity)

    await_arrivals(2, answered, capacity)

    for b in range(blocks):
        at = within(answered, index_s[2 * groups, b], 1)
        tab_c[b : b + 1, :] = answered[pl.ds(at, 1), :]
    coef[...] = tab_c[...].T
    advance(midway, coef, start_points, landed, time_step, 16)

    group = 8

    def basis(points, part, lanes, only=range(27)):
        lx = lagrange(points[0, part, lanes])
        ly = lagrange(points[1, part, lanes])
        lz = lagrange(points[2, part, lanes])
        for i, j in itertools.product(range(3), range(3)):
            nodes = [n for n in range(9 * i + 3 * j, 9 * i + 3 * j + 3) if n in only]
            if nodes:
                xy = lx[i] * ly[j]
                for n in nodes:
                    yield n, xy * lz[n % 3]

    def tabulate(only, group):
        def some(g, carry):
            part = pl.ds(pl.multiple_of(g * group, group), group)
            for n, value in basis(landed, part, slice(0, blocks), only):
                phi[n, part, :] = value
            return carry

        lax.fori_loop(0, markers // group, some, 0)

    def moments(nodes):
        def gather(g, sums):
            for s in range(8):
                m = g * 8 + s
                values = carried[pl.ds(pl.multiple_of(m * fields, fields), fields), :]
                sums = tuple(
                    total + phi[n, pl.ds(m, 1), :] * values for total, n in zip(sums, nodes)
                )
            return sums

        zero = jnp.zeros((fields, blocks), f32)
        sums = lax.fori_loop(0, markers // 8, gather, (zero,) * len(nodes))
        for index, total in enumerate(sums):
            table[index * fields : (index + 1) * fields, :] = total

    per_row = LANES // fields
    full = 27 // per_row
    last = tuple(range(full * per_row, 27))
    base = len(last) * fields
    half = LANES // 2
    tabulate(last, 32)
    moments(last)
    table[base:half, :] = jnp.zeros((half - base, blocks), f32)
    table[base : base + 1, :] = (elements[2:3, :] + 1).astype(f32)
    table[half:, :] = table[0:half, :]
    tab_t[0:blocks, :] = table[...].T
    place_tails(out_t, (tab_t, tab_t), index_s)
    exchange(4, out_t, in_t, shared)
    tabulate(range(full * per_row), group)
    moments(tuple(range(per_row)))
    tab_r[0:blocks, :] = table[...].T
    place_rows(out_r, tab_r, index_s, 0, 1)
    exchange(5, out_r, in_r, capacity)

    for j in range(2):
        moments(tuple(range((j + 1) * per_row, (j + 2) * per_row)))
        tab_e[pl.ds(j, blocks, stride=2), :] = table[...].T
    place_rows(out_e, tab_e, index_s, 1, 2)
    exchange(6, out_e, in_e, 2 * capacity)

    await_arrivals(1, in_a1, 2 * capacity)
    await_arrivals(3, in_a2, 2 * capacity)
    for part in range(wide_places // LANES):
        lanes = slice(part * LANES, (part + 1) * LANES)
        for c, (ref, row) in enumerate(((in_a1, 0), (in_a1, 1), (in_a2, 0))):
            points_m[c, :, lanes] = ref[pl.ds(2 * LANES * part + row, LANES, stride=2), :].T
        coef_m0[:, lanes] = in_a2[pl.ds(2 * LANES * part + 1, LANES, stride=2), :].T
        coef_m1[:, lanes] = answer[lanes, :].T
    advance(points_m, coef_m0, points_m, midway_m, 0.5 * time_step, 8)
    advance(midway_m, coef_m1, points_m, landed_m, time_step, 8)
    for part in range(wide_places // LANES):
        lanes = slice(part * LANES, (part + 1) * LANES)
        for c in range(3):
            tab_m[pl.ds(4 * LANES * part + c, LANES, stride=4), :] = landed_m[c, :, lanes].T
    turns.wait()
    place_rows(out_m, tab_m, turn_s, 2, 3)
    exchange(7, out_m, fin_m, 3 * capacity)

    await_arrivals(4, in_t, shared)
    tails = in_t[...]
    swapped = pltpu.roll(tails, half, 1)
    count = slots * shared
    for start, stride in parities(capacity):
        first_t[pl.ds(start, count, stride=stride), :] = swapped if start else tails
        second_t[pl.ds(start, count, stride=stride), :] = tails if start else swapped
    place_tails(on_t, (first_t, second_t), turn_s)
    exchange(8, on_t, fin_t, shared)
    await_arrivals(5, in_r, capacity)
    place_rows(on_r, in_r, turn_s, 0, 1)
    exchange(9, on_r, fin_r, capacity)
    await_arrivals(6, in_e, 2 * capacity)
    place_rows(on_e, in_e, turn_s, 1, 2)
    exchange(10, on_e, fin_e, 2 * capacity)

    await_arrivals(7, fin_m, 3 * capacity)
    halves = parities(capacity)
    count = places // len(halves)
    lanes_each = weights.shape[1] // len(halves)
    for index, (start, stride) in enumerate(halves):
        for c in range(3):
            tab_m[0:count, :] = fin_m[pl.ds(3 * start + c, count, stride=3 * stride), :]
            for part in range(lanes_each // LANES):
                at = index * lanes_each + part * LANES
                points_m[c, :, at : at + LANES] = tab_m[part * LANES : (part + 1) * LANES, :].T
    for part in range(weights.shape[1] // LANES):
        lanes = slice(part * LANES, (part + 1) * LANES)

        def square(g, sums, lanes=lanes):
            part = pl.ds(pl.multiple_of(g * group, group), group)
            return tuple(sums[n] + value * value for n, value in basis(points_m, part, lanes))

        zero = jnp.zeros((group, LANES), f32)
        sums = lax.fori_loop(0, markers // group, square, (zero,) * 27)
        for n in range(27):
            weights[n : n + 1, lanes] = jnp.sum(sums[n], axis=0, keepdims=True)
        weights[27:, lanes] = jnp.zeros((weights.shape[0] - 27, LANES), f32)

    await_arrivals(8, fin_t, shared)
    await_arrivals(9, fin_r, capacity)
    await_arrivals(10, fin_e, 2 * capacity)
    await_sends(0, request, 1)
    await_sends(1, out_a1, 2 * capacity)
    await_sends(2, answer, capacity)
    await_sends(3, out_a2, 2 * capacity)
    await_sends(4, out_t, shared)
    await_sends(5, out_r, capacity)
    await_sends(6, out_e, 2 * capacity)
    await_sends(7, out_m, 3 * capacity)
    await_sends(8, on_t, shared)
    await_sends(9, on_r, capacity)
    await_sends(10, on_e, 2 * capacity)


def settle(fields, capacity, landed, tails, first, rest, weights, moved, projected):
    owned = projected.shape[2]
    places = landed.shape[0] // 3
    per_row = LANES // fields
    full = 27 // per_row
    base = (27 - full * per_row) * fields
    half = LANES // 2
    for c in range(3):
        moved[c] = landed[pl.ds(c, places, stride=3), :]
    halves = parities(capacity)
    count = places // len(halves)
    lanes_each = weights.shape[1] // len(halves)
    hits = []
    for index in range(len(halves)):
        at = index * half + base
        element = tails[:, at : at + 1].astype(i32)
        hits.append(mask(iota((count, owned), 1) + 1 == element))

    def total(lines, index):
        high, low = split(lines)
        return dot(high, hits[index], ((1,), (0,))) + dot(low, hits[index], ((1,), (0,)))

    def summed(lines):
        return functools.reduce(jnp.add, [total(l, index) for index, l in enumerate(lines)])

    lanes = [slice(index * lanes_each, index * lanes_each + count) for index in range(len(halves))]
    inverse = 1.0 / (1.0 + summed([weights[:, l] for l in lanes]))
    turned = tails[...].T
    ends = summed([turned[index * half : (index + 1) * half] for index in range(len(halves))])
    node = 0
    for j in range(full):
        ref, row, rows = ((first, 0, 1), (rest, 0, 2), (rest, 1, 2))[j]
        sums = summed(
            [ref[pl.ds(rows * start + row, count, stride=rows * stride), :].T
             for start, stride in halves]
        )
        for n in range(per_row):
            projected[node] = sums[n * fields : (n + 1) * fields, :] * inverse[node : node + 1, :]
            node += 1
    for n in range(27 - node):
        projected[node + n] = (
            ends[n * fields : (n + 1) * fields, :] * inverse[node + n : node + n + 1, :]
        )


def per_device(n_lat, n_rad, positions, fields, velocity, counts, elements, routes):
    blocks, _, markers = positions.shape
    n_fields = fields.shape[1]
    capacity = max(1, 2 * blocks // (3 * n_rad))
    slots = 3 * n_rad
    places = slots * capacity
    shared = slots * ((capacity + 1) // 2)
    owned = velocity.shape[1]
    wide_places = round_up(places + 1, LANES)
    halves = len(parities(capacity))
    weight_lanes = halves * round_up(places // halves, LANES)
    vmem = pl.BlockSpec(memory_space=pltpu.VMEM)
    anywhere = pl.BlockSpec(memory_space=pltpu.HBM)

    def rows(n):
        return pltpu.VMEM((round_up(n, 8), LANES), f32)

    def looked_up(n, each):
        return rows((1 << (n * each).bit_length()) + each)

    small = pltpu.VMEM((slots, 2, LANES), f32)
    points = pltpu.VMEM((3, markers, blocks), f32)
    wide_points = pltpu.VMEM((3, markers, wide_places), f32)
    square = pltpu.VMEM((LANES, LANES), f32)
    together = max(n for n in range(1, 5) if slots % n == 0)
    index_rows = 3 * round_up(slots // together, 8)
    index = pltpu.VMEM((index_rows, LANES), i32)
    index_s = pltpu.SMEM((index_rows, LANES), i32)
    final_rows = (3 * places, shared, places, 2 * places)
    inputs = (jnp.transpose(positions, (1, 0, 2)), velocity, elements, routes, fields)
    final = pl.pallas_call(
        functools.partial(trip, n_lat, n_rad, capacity),
        out_shape=[jax.ShapeDtypeStruct((n, LANES), f32) for n in final_rows]
        + [jax.ShapeDtypeStruct((32, weight_lanes), f32)],
        in_specs=[pl.BlockSpec(memory_space=pltpu.SMEM)] + [anywhere] * 5,
        out_specs=[vmem] * 5,
        scratch_shapes=[
            pltpu.VMEM((3, blocks, markers), f32),
            pltpu.VMEM(velocity.shape, f32),
            pltpu.VMEM(elements.shape, i32),
            pltpu.VMEM(routes.shape, i32),
            pltpu.VMEM(fields.shape, fields.dtype),
            rows((blocks + 1) * n_fields), rows((markers + 1) * n_fields),
            points, points, points,
            square,
            pltpu.VMEM((27, markers, blocks), f32),
            square,
            looked_up(blocks, 2), looked_up(blocks, 2),
            looked_up(blocks, 1), looked_up(blocks, 1), looked_up(blocks, 2),
            square, looked_up(wide_places - 1, 4),
            looked_up(places, 1), looked_up(places, 1),
            wide_points, wide_points, wide_points,
            pltpu.VMEM((LANES, wide_places), f32), pltpu.VMEM((LANES, wide_places), f32),
            small, small,
            rows(2 * places), rows(2 * wide_places + 8),
            rows(2 * places), rows(2 * wide_places + 8),
            rows(wide_places), looked_up(places, 1), rows(3 * places),
            rows(shared), rows(shared), rows(shared),
            rows(places), looked_up(places, 1), rows(places),
            rows(2 * places), looked_up(places, 2), rows(2 * places),
            index, index, index_s, index_s,
            pltpu.SemaphoreType.DMA((8,)),
            pltpu.SemaphoreType.DMA((11,)),
            pltpu.SemaphoreType.DMA((11,)),
        ],
        compiler_params=pltpu.CompilerParams(
            collective_id=0, has_side_effects=True, vmem_limit_bytes=24 * 1024 * 1024
        ),
        name="trip",
    )(counts, *[pltpu.with_memory_space_constraint(x, pltpu.HBM) for x in inputs])
    moved, projected = pl.pallas_call(
        functools.partial(settle, n_fields, capacity),
        out_shape=(
            jax.ShapeDtypeStruct((3, places, markers), f32),
            jax.ShapeDtypeStruct((27, n_fields, owned), f32),
        ),
        in_specs=[vmem] * 5,
        out_specs=(vmem, vmem),
        compiler_params=pltpu.CompilerParams(vmem_limit_bytes=16 * 1024 * 1024),
        name="settle",
    )(*final)
    return jnp.transpose(moved, (1, 0, 2)), projected


def solution(mesh):
    in_specs = (
        P(("lat", "rad"), None, None),
        P(("lat", "rad"), None, None),
        P(None, ("lat", "rad")),
        P(("lat", "rad")),
        P(None, ("lat", "rad")),
        P(None, ("lat", "rad")),
    )
    out_specs = (P(("lat", "rad"), None, None), P(None, None, ("lat", "rad")))
    return jax.shard_map(
        functools.partial(per_device, mesh.shape["lat"], mesh.shape["rad"]),
        mesh=mesh, in_specs=in_specs, out_specs=out_specs, check_vma=False,
    )
```

```python
import functools
import itertools

import jax
import jax.numpy as jnp
from jax import lax
from jax.experimental import pallas as pl
from jax.experimental.pallas import tpu as pltpu
from jax.sharding import PartitionSpec as P

time_step = 0.4
MESH = pl.DeviceIdType.MESH
LANES = 128
bf16, f32, i32 = jnp.bfloat16, jnp.float32, jnp.int32


def round_up(x, by):
    return -(-x // by) * by


def split(x):
    high = x.astype(bf16)
    low = (x - high.astype(f32)).astype(bf16)
    return high, low


def dot(a, b, dims):
    return lax.dot_general(a, b, (dims, ((), ())), preferred_element_type=f32)


def iota(shape, axis):
    return lax.broadcasted_iota(i32, shape, axis)


def mask(condition):
    return condition.astype(f32).astype(bf16)


def lagrange(s):
    return (2.0 * (s - 0.5) * (s - 1.0), -4.0 * s * (s - 1.0), 2.0 * s * (s - 0.5))


def advance(points_in, coefficients, base, out, scale, group):
    markers = base.shape[1]

    def step(g, carry):
        rows = pl.ds(pl.multiple_of(g * group, group), group)
        lx = lagrange(points_in[0, rows, :])
        ly = lagrange(points_in[1, rows, :])
        lz = lagrange(points_in[2, rows, :])
        sums = [None] * 3
        for i in range(3):
            inner = [None] * 3
            for j in range(3):
                for c in range(3):
                    n = c * 27 + 9 * i + 3 * j
                    line = (
                        coefficients[n : n + 1, :] * lz[0]
                        + coefficients[n + 1 : n + 2, :] * lz[1]
                        + coefficients[n + 2 : n + 3, :] * lz[2]
                    ) * ly[j]
                    inner[c] = line if inner[c] is None else inner[c] + line
            for c in range(3):
                term = inner[c] * lx[i]
                sums[c] = term if sums[c] is None else sums[c] + term
        for c in range(3):
            out[c, rows, :] = base[c, rows, :] + scale * sums[c]
        return carry

    lax.fori_loop(0, markers // group, step, 0)


def parities(capacity):
    return ((0, 2), (1, 2)) if capacity % 2 == 0 else ((0, 1),)


def hits_of(tails, halves, count, owned, base):
    hits = []
    for index in range(len(halves)):
        at = index * (LANES // 2) + base
        element = tails[:, at : at + 1].astype(i32)
        hits.append(mask(iota((count, owned), 1) + 1 == element))
    return hits


def summed(lines, hits):
    total = None
    for line, hit in zip(lines, hits):
        high, low = split(line)
        part = dot(high, hit, ((1,), (0,))) + dot(low, hit, ((1,), (0,)))
        total = part if total is None else total + part
    return total


def trip(
    n_lat, n_rad, capacity,
    counts, pos_in, vel_in, elements_in, routes_in, fld_in,
    fin_t, fin_e, moved, early, inverse,
    pos, vel, elements, routes, raw, wide, carried,
    start_points, midway, landed, coef, phi, table,
    tab_a1, tab_a2, tab_t, tab_r, tab_e, tab_c, tab_m, first_t, second_t,
    points_m, midway_m, landed_m, coef_m0, coef_m1,
    request, asked, out_a1, in_a1, out_a2, in_a2, answer, answered, out_m,
    out_t, in_t, on_t, out_r, in_r, on_r, out_e, in_e, on_e, fin_m, fin_r, weights,
    index_v, turn_v, index_s, turn_s,
    load_sem, send_sem, recv_sem,
):
    lat, rad = lax.axis_index("lat"), lax.axis_index("rad")
    slots = 3 * n_rad
    places = slots * capacity
    shared = (capacity + 1) // 2
    together = max(n for n in range(1, 5) if slots % n == 0)
    groups = round_up(slots // together, 8)
    blocks, fields, markers = fld_in.shape
    n_vel, owned = vel.shape
    wide_places = points_m.shape[2]

    def load(index, source, target):
        copy = pltpu.make_async_copy(source, target, load_sem.at[index])
        copy.start()
        return copy

    load_routes = load(0, routes_in, routes)
    load_elements = load(1, elements_in, elements)
    load_pos = load(2, pos_in, pos)
    load_vel = load(3, vel_in, vel)
    load_fld = load(4, fld_in, raw)

    def partner(k, q, back):
        by = (1 - k) if back else (k - 1)
        return lax.rem(lat + by + n_lat, n_lat), q

    def outward(back):
        first = 2 * (2 * lat // n_lat)
        return enumerate((2 - first, first, 1) if back else (first, 2 - first, 1))

    barrier = pltpu.get_barrier_semaphore()
    for place, k in outward(False):

        def greet(dq, carry, k=k):
            q = lax.rem(rad + dq, n_rad)
            pl.semaphore_signal(
                barrier, inc=1, device_id=partner(k, q, False), device_id_type=MESH
            )
            return carry

        lax.fori_loop(int(place == 2), n_rad, greet, 0)

    def exchange(phase, source, target, size, back=False):
        for place, k in outward(back):

            def send(dq, carry, k=k, place=place):
                q = lax.rem(rad + dq, n_rad)
                if phase >= 10:
                    q = dq - 1 + (dq - 1 + n_rad - rad) // n_rad if place == 2 else dq
                pltpu.make_async_remote_copy(
                    src_ref=source.at[pl.ds((k * n_rad + q) * size, size)],
                    dst_ref=target.at[pl.ds((k * n_rad + rad) * size, size)],
                    send_sem=send_sem.at[phase],
                    recv_sem=recv_sem.at[phase],
                    device_id=partner(k, q, back),
                    device_id_type=MESH,
                ).start()
                return carry

            lax.fori_loop(int(place == 2), n_rad, send, 0)
        own = pl.ds((n_rad + rad) * size, size)
        pltpu.make_async_copy(source.at[own], target.at[own], recv_sem.at[phase]).start()

    def await_arrivals(phase, target, size):
        part = target.at[pl.ds(0, slots * size)]
        pltpu.make_async_copy(part, part, recv_sem.at[phase]).wait()

    def await_sends(phase, source, size):
        part = source.at[pl.ds(0, (slots - 1) * size)]
        pltpu.make_async_copy(part, part, send_sem.at[phase]).wait()

    def slot_of(place, each=capacity):
        return jnp.floor((place.astype(f32) + 0.5) * (1.0 / each)).astype(i32)

    def grouped(place):
        group = slot_of(place, capacity * together)
        return group, place - group * (capacity * together)

    def within(source, at, rows):
        bits = (source.shape[0] - rows + 1).bit_length() - 1
        return at & ((1 << bits) - 1)

    def place_rows(out, source, indices, row, rows):
        at_once = capacity * together

        def some(g, carry):
            for c in range(at_once):
                p = g * at_once + c
                at = within(source, indices[row * groups + g, c], rows)
                out[pl.ds(p * rows, rows), :] = source[pl.ds(at, rows), :]
            return carry

        lax.fori_loop(0, slots // together, some, 0)

    def place_tails(out, sources, indices):
        lower = iota((1, LANES), 1) < LANES // 2

        def some(g, carry):
            for s, pair in itertools.product(range(together), range(shared)):
                halves = []
                for half, source in enumerate(sources):
                    c = s * capacity + min(2 * pair + half, capacity - 1)
                    at = within(source, indices[g, c], 1)
                    halves.append(source[pl.ds(at, 1), :])
                line = jnp.where(lower, halves[0], halves[1])
                out[pl.ds((g * together + s) * shared + pair, 1), :] = line
            return carry

        lax.fori_loop(0, slots // together, some, 0)

    def clear(ref, start):
        ref[start:, :] = jnp.zeros((ref.shape[0] - start, LANES), f32)

    for ref, start in (
        (tab_a1, 2 * blocks), (tab_a2, 2 * blocks), (tab_t, blocks), (tab_r, blocks),
        (tab_e, 2 * blocks), (in_a1, 2 * places), (in_a2, 2 * places), (first_t, places),
        (second_t, places), (in_r, places), (in_e, 2 * places), (answer, 0), (coef, 0),
    ):
        clear(ref, start)
    index_v[...] = jnp.zeros(index_v.shape, i32)
    turn_v[...] = jnp.zeros(turn_v.shape, i32)

    load_routes.wait()
    load_elements.wait()
    route = jnp.where(iota((1, blocks), 1) < counts[0], routes[0:1, :], -1)
    slot = slot_of(route)
    sent_to = iota((slots, blocks), 0) == slot
    inside = mask(iota((LANES, blocks), 0) == route - slot * capacity)
    for row, label in enumerate((elements[1:2, :], routes[1:2, :])):
        marked = jnp.where(sent_to, (label + 1).astype(f32), 0.0).astype(bf16)
        request[:, row, :] = dot(marked, inside, ((1,), (1,)))
    group_of, within_group = grouped(route)
    chosen = iota((groups, blocks), 0) == group_of
    numbers = iota((groups, blocks), 1) - blocks
    numbers = jnp.where(chosen, numbers.astype(f32), 0.0).astype(bf16)
    matched = mask(iota((LANES, blocks), 0) == within_group)
    holder = (dot(numbers, matched, ((1,), (1,))) + float(blocks)).astype(i32)
    for row in range(2):
        index_v[row * groups : (row + 1) * groups, :] = holder * (1 << row)
    index_v[2 * groups : 2 * groups + 1, 0:blocks] = jnp.maximum(route, 0)
    indices = load(5, index_v, index_s)
    load_pos.wait()
    for c in range(2):
        tab_a1[pl.ds(c, blocks, stride=2), :] = pos[c]
    tab_a2[pl.ds(0, blocks, stride=2), :] = pos[2]
    indices.wait()
    place_rows(out_a1, tab_a1, index_s, 1, 2)
    pl.semaphore_wait(barrier, slots - 1)
    exchange(0, request, asked, 1)
    exchange(1, out_a1, in_a1, 2 * capacity)

    load_vel.wait()
    vel_high, vel_low = split(vel[...])
    pick = mask(iota((owned, blocks), 0) == elements[0:1, :])
    coef[0:n_vel, :] = dot(vel_high, pick, ((1,), (0,))) + dot(vel_low, pick, ((1,), (0,)))
    tab_a2[pl.ds(1, blocks, stride=2), :] = coef[...].T
    place_rows(out_a2, tab_a2, index_s, 1, 2)

    for c in range(3):
        start_points[c] = pos[c].T
    advance(start_points, coef, start_points, midway, 0.5 * time_step, 16)

    own_slot = slot_of(iota((places, slots), 0))
    by_slot = mask(own_slot == iota((places, slots), 1))
    lane = iota((places, LANES), 0) - slot_of(iota((places, LANES), 0)) * capacity
    by_lane = lane == iota((places, LANES), 1)

    def label_column(row):
        lines = dot(by_slot, asked[:, row, :].astype(bf16), ((1,), (0,)))
        return jnp.sum(jnp.where(by_lane, lines, 0.0), axis=1, keepdims=True).astype(i32)

    await_arrivals(0, asked, 1)
    pick = mask(iota((places, owned), 1) + 1 == label_column(0))
    answer[0:places, 0:n_vel] = dot(pick, vel_high, ((1,), (1,))) + dot(
        pick, vel_low, ((1,), (1,))
    )
    exchange(2, answer, answered, capacity, back=True)

    group_of, within_group = grouped(label_column(1) - 1)
    chosen = iota((places, LANES), 1) == group_of
    numbers = iota((places, LANES), 0) - places
    numbers = jnp.where(chosen, numbers.astype(f32), 0.0).astype(bf16)
    matched = mask(iota((places, LANES), 1) == within_group)
    holder = (dot(numbers, matched, ((0,), (0,))) + float(places)).astype(i32)
    for row in range(3):
        turn_v[row * groups : (row + 1) * groups, :] = holder[0:groups, :] * (1 << row)
    turns = load(6, turn_v, turn_s)
    load_fld.wait()
    wide[0 : blocks * fields, :] = raw[...].astype(f32).reshape(blocks * fields, markers)
    for f in range(fields):
        carried[pl.ds(f, markers, stride=fields), :] = wide[pl.ds(f, blocks, stride=fields), :].T

    exchange(3, out_a2, in_a2, 2 * capacity)

    await_arrivals(2, answered, capacity)

    for b in range(blocks):
        at = within(answered, index_s[2 * groups, b], 1)
        tab_c[b : b + 1, :] = answered[pl.ds(at, 1), :]
    coef[...] = tab_c[...].T
    advance(midway, coef, start_points, landed, time_step, 16)

    group = 8

    def basis(points, part, lanes, only=range(27)):
        lx = lagrange(points[0, part, lanes])
        ly = lagrange(points[1, part, lanes])
        lz = lagrange(points[2, part, lanes])
        for i, j in itertools.product(range(3), range(3)):
            nodes = [n for n in range(9 * i + 3 * j, 9 * i + 3 * j + 3) if n in only]
            if nodes:
                xy = lx[i] * ly[j]
                for n in nodes:
                    yield n, xy * lz[n % 3]

    def tabulate(only, group):
        def some(g, carry):
            part = pl.ds(pl.multiple_of(g * group, group), group)
            for n, value in basis(landed, part, slice(0, blocks), only):
                phi[n, part, :] = value
            return carry

        lax.fori_loop(0, markers // group, some, 0)

    def moments(nodes):
        def gather(g, sums):
            for s in range(8):
                m = g * 8 + s
                values = carried[pl.ds(pl.multiple_of(m * fields, fields), fields), :]
                sums = tuple(
                    total + phi[n, pl.ds(m, 1), :] * values for total, n in zip(sums, nodes)
                )
            return sums

        zero = jnp.zeros((fields, blocks), f32)
        sums = lax.fori_loop(0, markers // 8, gather, (zero,) * len(nodes))
        for index, total in enumerate(sums):
            table[index * fields : (index + 1) * fields, :] = total

    per_row = LANES // fields
    full = 27 // per_row
    last = tuple(range(full * per_row, 27))
    base = len(last) * fields
    half = LANES // 2
    tabulate(last, 32)
    moments(last)
    table[base:half, :] = jnp.zeros((half - base, blocks), f32)
    table[base : base + 1, :] = (elements[2:3, :] + 1).astype(f32)
    table[half:, :] = table[0:half, :]
    tab_t[0:blocks, :] = table[...].T
    place_tails(out_t, (tab_t, tab_t), index_s)
    exchange(4, out_t, in_t, shared)
    tabulate(range(full * per_row), group)
    moments(tuple(range(per_row)))
    tab_r[0:blocks, :] = table[...].T
    place_rows(out_r, tab_r, index_s, 0, 1)
    exchange(5, out_r, in_r, capacity)

    for j in range(2):
        moments(tuple(range((j + 1) * per_row, (j + 2) * per_row)))
        tab_e[pl.ds(j, blocks, stride=2), :] = table[...].T
    place_rows(out_e, tab_e, index_s, 1, 2)
    exchange(6, out_e, in_e, 2 * capacity)

    await_arrivals(1, in_a1, 2 * capacity)
    await_arrivals(3, in_a2, 2 * capacity)
    for part in range(wide_places // LANES):
        lanes = slice(part * LANES, (part + 1) * LANES)
        for c, (ref, row) in enumerate(((in_a1, 0), (in_a1, 1), (in_a2, 0))):
            points_m[c, :, lanes] = ref[pl.ds(2 * LANES * part + row, LANES, stride=2), :].T
        coef_m0[:, lanes] = in_a2[pl.ds(2 * LANES * part + 1, LANES, stride=2), :].T
        coef_m1[:, lanes] = answer[lanes, :].T
    advance(points_m, coef_m0, points_m, midway_m, 0.5 * time_step, 8)
    advance(midway_m, coef_m1, points_m, landed_m, time_step, 8)
    for part in range(wide_places // LANES):
        lanes = slice(part * LANES, (part + 1) * LANES)
        for c in range(3):
            tab_m[pl.ds(4 * LANES * part + c, LANES, stride=4), :] = landed_m[c, :, lanes].T
    turns.wait()
    place_rows(out_m, tab_m, turn_s, 2, 3)
    exchange(7, out_m, fin_m, 3 * capacity)

    await_arrivals(4, in_t, shared)
    tails = in_t[...]
    swapped = pltpu.roll(tails, half, 1)
    count = slots * shared
    for start, stride in parities(capacity):
        first_t[pl.ds(start, count, stride=stride), :] = swapped if start else tails
        second_t[pl.ds(start, count, stride=stride), :] = tails if start else swapped
    place_tails(on_t, (first_t, second_t), turn_s)
    exchange(8, on_t, fin_t, shared)
    await_arrivals(5, in_r, capacity)
    place_rows(on_r, in_r, turn_s, 0, 1)
    exchange(9, on_r, fin_r, capacity)
    await_arrivals(6, in_e, 2 * capacity)
    place_rows(on_e, in_e, turn_s, 1, 2)
    exchange(10, on_e, fin_e, 2 * capacity)

    await_arrivals(7, fin_m, 3 * capacity)
    halves = parities(capacity)
    count = places // len(halves)
    lanes_each = weights.shape[1] // len(halves)
    for index, (start, stride) in enumerate(halves):
        for c in range(3):
            tab_m[0:count, :] = fin_m[pl.ds(3 * start + c, count, stride=3 * stride), :]
            for part in range(lanes_each // LANES):
                at = index * lanes_each + part * LANES
                points_m[c, :, at : at + LANES] = tab_m[part * LANES : (part + 1) * LANES, :].T
    for part in range(weights.shape[1] // LANES):
        lanes = slice(part * LANES, (part + 1) * LANES)

        def square(g, sums, lanes=lanes):
            part = pl.ds(pl.multiple_of(g * group, group), group)
            return tuple(sums[n] + value * value for n, value in basis(points_m, part, lanes))

        zero = jnp.zeros((group, LANES), f32)
        sums = lax.fori_loop(0, markers // group, square, (zero,) * 27)
        for n in range(27):
            weights[n : n + 1, lanes] = jnp.sum(sums[n], axis=0, keepdims=True)
        weights[27:, lanes] = jnp.zeros((weights.shape[0] - 27, LANES), f32)

    for c in range(3):
        moved[c] = fin_m[pl.ds(c, places, stride=3), :]
    await_arrivals(8, fin_t, shared)
    hits = hits_of(fin_t, halves, places // len(halves), owned, base)
    sums = summed(
        [weights[:, at * lanes_each : at * lanes_each + count] for at in range(len(halves))], hits
    )
    inverse[...] = 1.0 / (1.0 + sums)
    turned = fin_t[...].T
    sums = summed([turned[at * half : (at + 1) * half] for at in range(len(halves))], hits)
    for n in range(len(last)):
        node = full * per_row + n
        early[per_row + n] = sums[n * fields : (n + 1) * fields] * inverse[node : node + 1, :]
    await_arrivals(9, fin_r, capacity)
    sums = summed([fin_r[pl.ds(start, count, stride=stride), :].T for start, stride in halves], hits)
    for n in range(per_row):
        early[n] = sums[n * fields : (n + 1) * fields] * inverse[n : n + 1, :]

    await_arrivals(10, fin_e, 2 * capacity)
    await_sends(0, request, 1)
    await_sends(1, out_a1, 2 * capacity)
    await_sends(2, answer, capacity)
    await_sends(3, out_a2, 2 * capacity)
    await_sends(4, out_t, shared)
    await_sends(5, out_r, capacity)
    await_sends(6, out_e, 2 * capacity)
    await_sends(7, out_m, 3 * capacity)
    await_sends(8, on_t, shared)
    await_sends(9, on_r, capacity)
    await_sends(10, on_e, 2 * capacity)


def settle(
    fields, places, base, halves, tails, rest, moved, early, inverse, moved_out, projected_out,
    projected, sems,
):
    owned = projected.shape[2]
    per_row = LANES // fields
    n_late = projected.shape[0]

    def write(index, source, target):
        copy = pltpu.make_async_copy(source, target, sems.at[index])
        copy.start()
        return copy

    n_last = early.shape[0] - per_row
    copies = [
        write(0, early.at[pl.ds(0, per_row)], projected_out.at[pl.ds(0, per_row)]),
        write(1, early.at[pl.ds(per_row, n_last)], projected_out.at[pl.ds(per_row + n_late, n_last)]),
        write(2, moved, moved_out),
    ]
    count = places // len(halves)
    hits = hits_of(tails, halves, count, owned, base)
    for j in range(n_late // per_row):
        sums = summed(
            [rest[pl.ds(2 * start + j, count, stride=2 * stride), :].T for start, stride in halves],
            hits,
        )
        for n in range(per_row):
            node = (j + 1) * per_row + n
            projected[j * per_row + n] = (
                sums[n * fields : (n + 1) * fields, :] * inverse[node : node + 1, :]
            )
        copies.append(
            write(
                3 + j,
                projected.at[pl.ds(j * per_row, per_row)],
                projected_out.at[pl.ds((j + 1) * per_row, per_row)],
            )
        )
    for copy in copies:
        copy.wait()


def per_device(n_lat, n_rad, positions, fields, velocity, counts, elements, routes):
    blocks, _, markers = positions.shape
    n_fields = fields.shape[1]
    capacity = max(1, 2 * blocks // (3 * n_rad))
    slots = 3 * n_rad
    places = slots * capacity
    shared = slots * ((capacity + 1) // 2)
    owned = velocity.shape[1]
    wide_places = round_up(places + 1, LANES)
    halves = len(parities(capacity))
    weight_lanes = halves * round_up(places // halves, LANES)
    vmem = pl.BlockSpec(memory_space=pltpu.VMEM)
    anywhere = pl.BlockSpec(memory_space=pltpu.HBM)

    def rows(n):
        return pltpu.VMEM((round_up(n, 8), LANES), f32)

    def looked_up(n, each):
        return rows((1 << (n * each).bit_length()) + each)

    small = pltpu.VMEM((slots, 2, LANES), f32)
    points = pltpu.VMEM((3, markers, blocks), f32)
    wide_points = pltpu.VMEM((3, markers, wide_places), f32)
    square = pltpu.VMEM((LANES, LANES), f32)
    together = max(n for n in range(1, 5) if slots % n == 0)
    index_rows = 3 * round_up(slots // together, 8)
    index = pltpu.VMEM((index_rows, LANES), i32)
    index_s = pltpu.SMEM((index_rows, LANES), i32)
    per_row = LANES // n_fields
    n_last = 27 % per_row
    inputs = (jnp.transpose(positions, (1, 0, 2)), velocity, elements, routes, fields)
    final = pl.pallas_call(
        functools.partial(trip, n_lat, n_rad, capacity),
        out_shape=[
            jax.ShapeDtypeStruct(shape, f32)
            for shape in (
                (shared, LANES), (2 * places, LANES), (3, places, markers),
                (per_row + n_last, n_fields, owned), (32, owned),
            )
        ],
        in_specs=[pl.BlockSpec(memory_space=pltpu.SMEM)] + [anywhere] * 5,
        out_specs=[vmem] * 5,
        scratch_shapes=[
            pltpu.VMEM((3, blocks, markers), f32),
            pltpu.VMEM(velocity.shape, f32),
            pltpu.VMEM(elements.shape, i32),
            pltpu.VMEM(routes.shape, i32),
            pltpu.VMEM(fields.shape, fields.dtype),
            rows((blocks + 1) * n_fields), rows((markers + 1) * n_fields),
            points, points, points,
            square,
            pltpu.VMEM((27, markers, blocks), f32),
            square,
            looked_up(blocks, 2), looked_up(blocks, 2),
            looked_up(blocks, 1), looked_up(blocks, 1), looked_up(blocks, 2),
            square, looked_up(wide_places - 1, 4),
            looked_up(places, 1), looked_up(places, 1),
            wide_points, wide_points, wide_points,
            pltpu.VMEM((LANES, wide_places), f32), pltpu.VMEM((LANES, wide_places), f32),
            small, small,
            rows(2 * places), rows(2 * wide_places + 8),
            rows(2 * places), rows(2 * wide_places + 8),
            rows(wide_places), looked_up(places, 1), rows(3 * places),
            rows(shared), rows(shared), rows(shared),
            rows(places), looked_up(places, 1), rows(places),
            rows(2 * places), looked_up(places, 2), rows(2 * places),
            rows(3 * places), rows(places), pltpu.VMEM((32, weight_lanes), f32),
            index, index, index_s, index_s,
            pltpu.SemaphoreType.DMA((8,)),
            pltpu.SemaphoreType.DMA((11,)),
            pltpu.SemaphoreType.DMA((11,)),
        ],
        compiler_params=pltpu.CompilerParams(
            collective_id=0, has_side_effects=True, vmem_limit_bytes=24 * 1024 * 1024
        ),
        name="trip",
    )(counts, *[pltpu.with_memory_space_constraint(x, pltpu.HBM) for x in inputs])
    moved, projected = pl.pallas_call(
        functools.partial(settle, n_fields, places, n_last * n_fields, parities(capacity)),
        out_shape=(
            jax.ShapeDtypeStruct((3, places, markers), f32),
            jax.ShapeDtypeStruct((27, n_fields, owned), f32),
        ),
        in_specs=[vmem] * 5,
        out_specs=(anywhere, anywhere),
        scratch_shapes=[
            pltpu.VMEM((27 - per_row - n_last, n_fields, owned), f32),
            pltpu.SemaphoreType.DMA((27 // per_row + 2,)),
        ],
        compiler_params=pltpu.CompilerParams(vmem_limit_bytes=16 * 1024 * 1024),
        name="settle",
    )(*final)
    return jnp.transpose(moved, (1, 0, 2)), projected


def solution(mesh):
    in_specs = (
        P(("lat", "rad"), None, None),
        P(("lat", "rad"), None, None),
        P(None, ("lat", "rad")),
        P(("lat", "rad")),
        P(None, ("lat", "rad")),
        P(None, ("lat", "rad")),
    )
    out_specs = (P(("lat", "rad"), None, None), P(None, None, ("lat", "rad")))
    return jax.shard_map(
        functools.partial(per_device, mesh.shape["lat"], mesh.shape["rad"]),
        mesh=mesh, in_specs=in_specs, out_specs=out_specs, check_vma=False,
    )
```

```python
import functools
import itertools

import jax
import jax.numpy as jnp
from jax import lax
from jax.experimental import pallas as pl
from jax.experimental.pallas import tpu as pltpu
from jax.sharding import PartitionSpec as P

time_step = 0.4
MESH = pl.DeviceIdType.MESH
LANES = 128
bf16, f32, i32 = jnp.bfloat16, jnp.float32, jnp.int32


def round_up(x, by):
    return -(-x // by) * by


def split(x):
    high = x.astype(bf16)
    low = (x - high.astype(f32)).astype(bf16)
    return high, low


def dot(a, b, dims):
    return lax.dot_general(a, b, (dims, ((), ())), preferred_element_type=f32)


def iota(shape, axis):
    return lax.broadcasted_iota(i32, shape, axis)


def mask(condition):
    return condition.astype(f32).astype(bf16)


def lagrange(s):
    return (2.0 * (s - 0.5) * (s - 1.0), -4.0 * s * (s - 1.0), 2.0 * s * (s - 0.5))


def advance(points_in, coefficients, base, out, scale, group):
    markers = base.shape[1]

    def step(g, carry):
        rows = pl.ds(pl.multiple_of(g * group, group), group)
        lx = lagrange(points_in[0, rows, :])
        ly = lagrange(points_in[1, rows, :])
        lz = lagrange(points_in[2, rows, :])
        sums = [None] * 3
        for i in range(3):
            inner = [None] * 3
            for j in range(3):
                for c in range(3):
                    n = c * 27 + 9 * i + 3 * j
                    line = (
                        coefficients[n : n + 1, :] * lz[0]
                        + coefficients[n + 1 : n + 2, :] * lz[1]
                        + coefficients[n + 2 : n + 3, :] * lz[2]
                    ) * ly[j]
                    inner[c] = line if inner[c] is None else inner[c] + line
            for c in range(3):
                term = inner[c] * lx[i]
                sums[c] = term if sums[c] is None else sums[c] + term
        for c in range(3):
            out[c, rows, :] = base[c, rows, :] + scale * sums[c]
        return carry

    lax.fori_loop(0, markers // group, step, 0)


def parities(capacity):
    return ((0, 2), (1, 2)) if capacity % 2 == 0 else ((0, 1),)


def hits_of(tails, halves, count, owned, base):
    hits = []
    for index in range(len(halves)):
        at = index * (LANES // 2) + base
        element = tails[:, at : at + 1].astype(i32)
        hits.append(mask(iota((count, owned), 1) + 1 == element))
    return hits


def summed(lines, hits):
    total = None
    for line, hit in zip(lines, hits):
        high, low = split(line)
        part = dot(high, hit, ((1,), (0,))) + dot(low, hit, ((1,), (0,)))
        total = part if total is None else total + part
    return total


def trip(
    n_lat, n_rad, capacity,
    counts, pos_in, vel_in, elements_in, routes_in, fld_in,
    fin_t, fin_e, moved, early, inverse,
    pos, vel, elements, routes, raw, wide, carried,
    start_points, midway, landed, coef, phi, table,
    tab_a1, tab_a2, tab_t, tab_r, tab_e, tab_c, tab_m, first_t, second_t,
    points_m, midway_m, landed_m, coef_m0, coef_m1,
    request, asked, out_a1, in_a1, out_a2, in_a2, answer, answered, out_m,
    out_t, in_t, on_t, out_r, in_r, on_r, out_e, in_e, on_e, fin_m, fin_r, weights,
    index_v, turn_v, index_s, turn_s,
    load_sem, send_sem, recv_sem,
):
    lat, rad = lax.axis_index("lat"), lax.axis_index("rad")
    slots = 3 * n_rad
    places = slots * capacity
    shared = (capacity + 1) // 2
    together = max(n for n in range(1, 5) if slots % n == 0)
    groups = round_up(slots // together, 8)
    blocks, fields, markers = fld_in.shape
    n_vel, owned = vel.shape
    wide_places = points_m.shape[2]

    def load(index, source, target):
        copy = pltpu.make_async_copy(source, target, load_sem.at[index])
        copy.start()
        return copy

    load_routes = load(0, routes_in, routes)
    load_elements = load(1, elements_in, elements)
    load_pos = load(2, pos_in, pos)
    load_vel = load(3, vel_in, vel)
    load_fld = load(4, fld_in, raw)

    def partner(k, q, back):
        by = (1 - k) if back else (k - 1)
        return lax.rem(lat + by + n_lat, n_lat), q

    def outward(back):
        first = 2 * (2 * lat // n_lat)
        return enumerate((2 - first, first, 1) if back else (first, 2 - first, 1))

    barrier = pltpu.get_barrier_semaphore()
    for place, k in outward(False):

        def greet(dq, carry, k=k):
            q = lax.rem(rad + dq, n_rad)
            pl.semaphore_signal(
                barrier, inc=1, device_id=partner(k, q, False), device_id_type=MESH
            )
            return carry

        lax.fori_loop(int(place == 2), n_rad, greet, 0)

    def exchange(phase, source, target, size, back=False):
        for place, k in outward(back):

            def send(dq, carry, k=k, place=place):
                q = lax.rem(rad + dq, n_rad)
                if phase >= 10:
                    q = dq - 1 + (dq - 1 + n_rad - rad) // n_rad if place == 2 else dq
                pltpu.make_async_remote_copy(
                    src_ref=source.at[pl.ds((k * n_rad + q) * size, size)],
                    dst_ref=target.at[pl.ds((k * n_rad + rad) * size, size)],
                    send_sem=send_sem.at[phase],
                    recv_sem=recv_sem.at[phase],
                    device_id=partner(k, q, back),
                    device_id_type=MESH,
                ).start()
                return carry

            lax.fori_loop(int(place == 2), n_rad, send, 0)
        own = pl.ds((n_rad + rad) * size, size)
        pltpu.make_async_copy(source.at[own], target.at[own], recv_sem.at[phase]).start()

    def await_arrivals(phase, target, size):
        part = target.at[pl.ds(0, slots * size)]
        pltpu.make_async_copy(part, part, recv_sem.at[phase]).wait()

    def await_sends(phase, source, size):
        part = source.at[pl.ds(0, (slots - 1) * size)]
        pltpu.make_async_copy(part, part, send_sem.at[phase]).wait()

    def slot_of(place, each=capacity):
        return jnp.floor((place.astype(f32) + 0.5) * (1.0 / each)).astype(i32)

    def grouped(place):
        group = slot_of(place, capacity * together)
        return group, place - group * (capacity * together)

    def within(source, at, rows):
        bits = (source.shape[0] - rows + 1).bit_length() - 1
        return at & ((1 << bits) - 1)

    def place_rows(out, source, indices, row, rows):
        at_once = capacity * together

        def some(g, carry):
            for c in range(at_once):
                p = g * at_once + c
                at = within(source, indices[row * groups + g, c], rows)
                out[pl.ds(p * rows, rows), :] = source[pl.ds(at, rows), :]
            return carry

        lax.fori_loop(0, slots // together, some, 0)

    def place_tails(out, sources, indices):
        lower = iota((1, LANES), 1) < LANES // 2

        def some(g, carry):
            for s, pair in itertools.product(range(together), range(shared)):
                halves = []
                for half, source in enumerate(sources):
                    c = s * capacity + min(2 * pair + half, capacity - 1)
                    at = within(source, indices[g, c], 1)
                    halves.append(source[pl.ds(at, 1), :])
                line = jnp.where(lower, halves[0], halves[1])
                out[pl.ds((g * together + s) * shared + pair, 1), :] = line
            return carry

        lax.fori_loop(0, slots // together, some, 0)

    def clear(ref, start):
        ref[start:, :] = jnp.zeros((ref.shape[0] - start, LANES), f32)

    for ref, start in (
        (tab_a1, 2 * blocks), (tab_a2, 2 * blocks), (tab_t, blocks), (tab_r, blocks),
        (tab_e, 2 * blocks), (in_a1, 2 * places), (in_a2, 2 * places), (first_t, places),
        (second_t, places), (in_r, places), (in_e, 2 * places), (answer, 0), (coef, 0),
    ):
        clear(ref, start)
    index_v[...] = jnp.zeros(index_v.shape, i32)
    turn_v[...] = jnp.zeros(turn_v.shape, i32)

    load_routes.wait()
    load_elements.wait()
    route = jnp.where(iota((1, blocks), 1) < counts[0], routes[0:1, :], -1)
    slot = slot_of(route)
    sent_to = iota((slots, blocks), 0) == slot
    inside = mask(iota((LANES, blocks), 0) == route - slot * capacity)
    for row, label in enumerate((elements[1:2, :], routes[1:2, :])):
        marked = jnp.where(sent_to, (label + 1).astype(f32), 0.0).astype(bf16)
        request[:, row, :] = dot(marked, inside, ((1,), (1,)))
    group_of, within_group = grouped(route)
    chosen = iota((groups, blocks), 0) == group_of
    numbers = iota((groups, blocks), 1) - blocks
    numbers = jnp.where(chosen, numbers.astype(f32), 0.0).astype(bf16)
    matched = mask(iota((LANES, blocks), 0) == within_group)
    holder = (dot(numbers, matched, ((1,), (1,))) + float(blocks)).astype(i32)
    for row in range(2):
        index_v[row * groups : (row + 1) * groups, :] = holder * (1 << row)
    index_v[2 * groups : 2 * groups + 1, 0:blocks] = jnp.maximum(route, 0)
    indices = load(5, index_v, index_s)
    pl.semaphore_wait(barrier, slots - 1)
    exchange(0, request, asked, 1)
    load_pos.wait()
    for c in range(2):
        tab_a1[pl.ds(c, blocks, stride=2), :] = pos[c]
    tab_a2[pl.ds(0, blocks, stride=2), :] = pos[2]
    indices.wait()
    place_rows(out_a1, tab_a1, index_s, 1, 2)
    exchange(1, out_a1, in_a1, 2 * capacity)

    load_vel.wait()
    vel_high, vel_low = split(vel[...])
    pick = mask(iota((owned, blocks), 0) == elements[0:1, :])
    coef[0:n_vel, :] = dot(vel_high, pick, ((1,), (0,))) + dot(vel_low, pick, ((1,), (0,)))
    tab_a2[pl.ds(1, blocks, stride=2), :] = coef[...].T
    place_rows(out_a2, tab_a2, index_s, 1, 2)

    for c in range(3):
        start_points[c] = pos[c].T
    advance(start_points, coef, start_points, midway, 0.5 * time_step, 16)

    own_slot = slot_of(iota((places, slots), 0))
    by_slot = mask(own_slot == iota((places, slots), 1))
    lane = iota((places, LANES), 0) - slot_of(iota((places, LANES), 0)) * capacity
    by_lane = lane == iota((places, LANES), 1)

    def label_column(row):
        lines = dot(by_slot, asked[:, row, :].astype(bf16), ((1,), (0,)))
        return jnp.sum(jnp.where(by_lane, lines, 0.0), axis=1, keepdims=True).astype(i32)

    await_arrivals(0, asked, 1)
    pick = mask(iota((places, owned), 1) + 1 == label_column(0))
    answer[0:places, 0:n_vel] = dot(pick, vel_high, ((1,), (1,))) + dot(
        pick, vel_low, ((1,), (1,))
    )
    exchange(2, answer, answered, capacity, back=True)
    exchange(3, out_a2, in_a2, 2 * capacity)

    group_of, within_group = grouped(label_column(1) - 1)
    chosen = iota((places, LANES), 1) == group_of
    numbers = iota((places, LANES), 0) - places
    numbers = jnp.where(chosen, numbers.astype(f32), 0.0).astype(bf16)
    matched = mask(iota((places, LANES), 1) == within_group)
    holder = (dot(numbers, matched, ((0,), (0,))) + float(places)).astype(i32)
    for row in range(3):
        turn_v[row * groups : (row + 1) * groups, :] = holder[0:groups, :] * (1 << row)
    turns = load(6, turn_v, turn_s)
    load_fld.wait()
    wide[0 : blocks * fields, :] = raw[...].astype(f32).reshape(blocks * fields, markers)
    for f in range(fields):
        carried[pl.ds(f, markers, stride=fields), :] = wide[pl.ds(f, blocks, stride=fields), :].T


    await_arrivals(2, answered, capacity)

    for b in range(blocks):
        at = within(answered, index_s[2 * groups, b], 1)
        tab_c[b : b + 1, :] = answered[pl.ds(at, 1), :]
    coef[...] = tab_c[...].T
    advance(midway, coef, start_points, landed, time_step, 16)

    group = 8

    def basis(points, part, lanes, only=range(27)):
        lx = lagrange(points[0, part, lanes])
        ly = lagrange(points[1, part, lanes])
        lz = lagrange(points[2, part, lanes])
        for i, j in itertools.product(range(3), range(3)):
            nodes = [n for n in range(9 * i + 3 * j, 9 * i + 3 * j + 3) if n in only]
            if nodes:
                xy = lx[i] * ly[j]
                for n in nodes:
                    yield n, xy * lz[n % 3]

    def tabulate(only, group):
        def some(g, carry):
            part = pl.ds(pl.multiple_of(g * group, group), group)
            for n, value in basis(landed, part, slice(0, blocks), only):
                phi[n, part, :] = value
            return carry

        lax.fori_loop(0, markers // group, some, 0)

    def moments(nodes):
        def gather(g, sums):
            for s in range(8):
                m = g * 8 + s
                values = carried[pl.ds(pl.multiple_of(m * fields, fields), fields), :]
                sums = tuple(
                    total + phi[n, pl.ds(m, 1), :] * values for total, n in zip(sums, nodes)
                )
            return sums

        zero = jnp.zeros((fields, blocks), f32)
        sums = lax.fori_loop(0, markers // 8, gather, (zero,) * len(nodes))
        for index, total in enumerate(sums):
            table[index * fields : (index + 1) * fields, :] = total

    per_row = LANES // fields
    full = 27 // per_row
    last = tuple(range(full * per_row, 27))
    base = len(last) * fields
    half = LANES // 2
    tabulate(last, 32)
    moments(last)
    table[base:half, :] = jnp.zeros((half - base, blocks), f32)
    table[base : base + 1, :] = (elements[2:3, :] + 1).astype(f32)
    table[half:, :] = table[0:half, :]
    tab_t[0:blocks, :] = table[...].T
    place_tails(out_t, (tab_t, tab_t), index_s)
    exchange(4, out_t, in_t, shared)
    tabulate(range(full * per_row), group)
    moments(tuple(range(per_row)))
    tab_r[0:blocks, :] = table[...].T
    place_rows(out_r, tab_r, index_s, 0, 1)
    exchange(5, out_r, in_r, capacity)

    for j in range(2):
        moments(tuple(range((j + 1) * per_row, (j + 2) * per_row)))
        tab_e[pl.ds(j, blocks, stride=2), :] = table[...].T
    place_rows(out_e, tab_e, index_s, 1, 2)
    exchange(6, out_e, in_e, 2 * capacity)

    await_arrivals(1, in_a1, 2 * capacity)
    await_arrivals(3, in_a2, 2 * capacity)
    for part in range(wide_places // LANES):
        lanes = slice(part * LANES, (part + 1) * LANES)
        for c, (ref, row) in enumerate(((in_a1, 0), (in_a1, 1), (in_a2, 0))):
            points_m[c, :, lanes] = ref[pl.ds(2 * LANES * part + row, LANES, stride=2), :].T
        coef_m0[:, lanes] = in_a2[pl.ds(2 * LANES * part + 1, LANES, stride=2), :].T
        coef_m1[:, lanes] = answer[lanes, :].T
    advance(points_m, coef_m0, points_m, midway_m, 0.5 * time_step, 8)
    advance(midway_m, coef_m1, points_m, landed_m, time_step, 8)
    for part in range(wide_places // LANES):
        lanes = slice(part * LANES, (part + 1) * LANES)
        for c in range(3):
            tab_m[pl.ds(4 * LANES * part + c, LANES, stride=4), :] = landed_m[c, :, lanes].T
    turns.wait()
    place_rows(out_m, tab_m, turn_s, 2, 3)
    exchange(7, out_m, fin_m, 3 * capacity)

    await_arrivals(4, in_t, shared)
    tails = in_t[...]
    swapped = pltpu.roll(tails, half, 1)
    count = slots * shared
    for start, stride in parities(capacity):
        first_t[pl.ds(start, count, stride=stride), :] = swapped if start else tails
        second_t[pl.ds(start, count, stride=stride), :] = tails if start else swapped
    place_tails(on_t, (first_t, second_t), turn_s)
    exchange(8, on_t, fin_t, shared)
    await_arrivals(5, in_r, capacity)
    place_rows(on_r, in_r, turn_s, 0, 1)
    exchange(9, on_r, fin_r, capacity)
    await_arrivals(6, in_e, 2 * capacity)
    place_rows(on_e, in_e, turn_s, 1, 2)
    exchange(10, on_e, fin_e, 2 * capacity)

    await_arrivals(7, fin_m, 3 * capacity)
    halves = parities(capacity)
    count = places // len(halves)
    lanes_each = weights.shape[1] // len(halves)
    for index, (start, stride) in enumerate(halves):
        for c in range(3):
            tab_m[0:count, :] = fin_m[pl.ds(3 * start + c, count, stride=3 * stride), :]
            for part in range(lanes_each // LANES):
                at = index * lanes_each + part * LANES
                points_m[c, :, at : at + LANES] = tab_m[part * LANES : (part + 1) * LANES, :].T
    for part in range(weights.shape[1] // LANES):
        lanes = slice(part * LANES, (part + 1) * LANES)

        def square(g, sums, lanes=lanes):
            part = pl.ds(pl.multiple_of(g * group, group), group)
            return tuple(sums[n] + value * value for n, value in basis(points_m, part, lanes))

        zero = jnp.zeros((group, LANES), f32)
        sums = lax.fori_loop(0, markers // group, square, (zero,) * 27)
        for n in range(27):
            weights[n : n + 1, lanes] = jnp.sum(sums[n], axis=0, keepdims=True)
        weights[27:, lanes] = jnp.zeros((weights.shape[0] - 27, LANES), f32)

    for c in range(3):
        moved[c] = fin_m[pl.ds(c, places, stride=3), :]
    await_arrivals(8, fin_t, shared)
    hits = hits_of(fin_t, halves, places // len(halves), owned, base)
    sums = summed(
        [weights[:, at * lanes_each : at * lanes_each + count] for at in range(len(halves))], hits
    )
    inverse[...] = 1.0 / (1.0 + sums)
    turned = fin_t[...].T
    sums = summed([turned[at * half : (at + 1) * half] for at in range(len(halves))], hits)
    for n in range(len(last)):
        node = full * per_row + n
        early[per_row + n] = sums[n * fields : (n + 1) * fields] * inverse[node : node + 1, :]
    await_arrivals(9, fin_r, capacity)
    sums = summed([fin_r[pl.ds(start, count, stride=stride), :].T for start, stride in halves], hits)
    for n in range(per_row):
        early[n] = sums[n * fields : (n + 1) * fields] * inverse[n : n + 1, :]

    await_arrivals(10, fin_e, 2 * capacity)
    await_sends(0, request, 1)
    await_sends(1, out_a1, 2 * capacity)
    await_sends(2, answer, capacity)
    await_sends(3, out_a2, 2 * capacity)
    await_sends(4, out_t, shared)
    await_sends(5, out_r, capacity)
    await_sends(6, out_e, 2 * capacity)
    await_sends(7, out_m, 3 * capacity)
    await_sends(8, on_t, shared)
    await_sends(9, on_r, capacity)
    await_sends(10, on_e, 2 * capacity)


def settle(
    fields, places, base, halves, tails, rest, moved, early, inverse, moved_out, projected_out,
    projected, sems,
):
    owned = projected.shape[2]
    per_row = LANES // fields
    n_late = projected.shape[0]

    def write(index, source, target):
        copy = pltpu.make_async_copy(source, target, sems.at[index])
        copy.start()
        return copy

    n_last = early.shape[0] - per_row
    copies = [
        write(0, early.at[pl.ds(0, per_row)], projected_out.at[pl.ds(0, per_row)]),
        write(1, early.at[pl.ds(per_row, n_last)], projected_out.at[pl.ds(per_row + n_late, n_last)]),
        write(2, moved, moved_out),
    ]
    count = places // len(halves)
    hits = hits_of(tails, halves, count, owned, base)
    for j in range(n_late // per_row):
        sums = summed(
            [rest[pl.ds(2 * start + j, count, stride=2 * stride), :].T for start, stride in halves],
            hits,
        )
        for n in range(per_row):
            node = (j + 1) * per_row + n
            projected[j * per_row + n] = (
                sums[n * fields : (n + 1) * fields, :] * inverse[node : node + 1, :]
            )
        copies.append(
            write(
                3 + j,
                projected.at[pl.ds(j * per_row, per_row)],
                projected_out.at[pl.ds((j + 1) * per_row, per_row)],
            )
        )
    for copy in copies:
        copy.wait()


def per_device(n_lat, n_rad, positions, fields, velocity, counts, elements, routes):
    blocks, _, markers = positions.shape
    n_fields = fields.shape[1]
    capacity = max(1, 2 * blocks // (3 * n_rad))
    slots = 3 * n_rad
    places = slots * capacity
    shared = slots * ((capacity + 1) // 2)
    owned = velocity.shape[1]
    wide_places = round_up(places + 1, LANES)
    halves = len(parities(capacity))
    weight_lanes = halves * round_up(places // halves, LANES)
    vmem = pl.BlockSpec(memory_space=pltpu.VMEM)
    anywhere = pl.BlockSpec(memory_space=pltpu.HBM)

    def rows(n):
        return pltpu.VMEM((round_up(n, 8), LANES), f32)

    def looked_up(n, each):
        return rows((1 << (n * each).bit_length()) + each)

    small = pltpu.VMEM((slots, 2, LANES), f32)
    points = pltpu.VMEM((3, markers, blocks), f32)
    wide_points = pltpu.VMEM((3, markers, wide_places), f32)
    square = pltpu.VMEM((LANES, LANES), f32)
    together = max(n for n in range(1, 5) if slots % n == 0)
    index_rows = 3 * round_up(slots // together, 8)
    index = pltpu.VMEM((index_rows, LANES), i32)
    index_s = pltpu.SMEM((index_rows, LANES), i32)
    per_row = LANES // n_fields
    n_last = 27 % per_row
    inputs = (jnp.transpose(positions, (1, 0, 2)), velocity, elements, routes, fields)
    final = pl.pallas_call(
        functools.partial(trip, n_lat, n_rad, capacity),
        out_shape=[
            jax.ShapeDtypeStruct(shape, f32)
            for shape in (
                (shared, LANES), (2 * places, LANES), (3, places, markers),
                (per_row + n_last, n_fields, owned), (32, owned),
            )
        ],
        in_specs=[pl.BlockSpec(memory_space=pltpu.SMEM)] + [anywhere] * 5,
        out_specs=[vmem] * 5,
        scratch_shapes=[
            pltpu.VMEM((3, blocks, markers), f32),
            pltpu.VMEM(velocity.shape, f32),
            pltpu.VMEM(elements.shape, i32),
            pltpu.VMEM(routes.shape, i32),
            pltpu.VMEM(fields.shape, fields.dtype),
            rows((blocks + 1) * n_fields), rows((markers + 1) * n_fields),
            points, points, points,
            square,
            pltpu.VMEM((27, markers, blocks), f32),
            square,
            looked_up(blocks, 2), looked_up(blocks, 2),
            looked_up(blocks, 1), looked_up(blocks, 1), looked_up(blocks, 2),
            square, looked_up(wide_places - 1, 4),
            looked_up(places, 1), looked_up(places, 1),
            wide_points, wide_points, wide_points,
            pltpu.VMEM((LANES, wide_places), f32), pltpu.VMEM((LANES, wide_places), f32),
            small, small,
            rows(2 * places), rows(2 * wide_places + 8),
            rows(2 * places), rows(2 * wide_places + 8),
            rows(wide_places), looked_up(places, 1), rows(3 * places),
            rows(shared), rows(shared), rows(shared),
            rows(places), looked_up(places, 1), rows(places),
            rows(2 * places), looked_up(places, 2), rows(2 * places),
            rows(3 * places), rows(places), pltpu.VMEM((32, weight_lanes), f32),
            index, index, index_s, index_s,
            pltpu.SemaphoreType.DMA((8,)),
            pltpu.SemaphoreType.DMA((11,)),
            pltpu.SemaphoreType.DMA((11,)),
        ],
        compiler_params=pltpu.CompilerParams(
            collective_id=0, has_side_effects=True, vmem_limit_bytes=24 * 1024 * 1024
        ),
        name="trip",
    )(counts, *[pltpu.with_memory_space_constraint(x, pltpu.HBM) for x in inputs])
    moved, projected = pl.pallas_call(
        functools.partial(settle, n_fields, places, n_last * n_fields, parities(capacity)),
        out_shape=(
            jax.ShapeDtypeStruct((3, places, markers), f32),
            jax.ShapeDtypeStruct((27, n_fields, owned), f32),
        ),
        in_specs=[vmem] * 5,
        out_specs=(anywhere, anywhere),
        scratch_shapes=[
            pltpu.VMEM((27 - per_row - n_last, n_fields, owned), f32),
            pltpu.SemaphoreType.DMA((27 // per_row + 2,)),
        ],
        compiler_params=pltpu.CompilerParams(vmem_limit_bytes=16 * 1024 * 1024),
        name="settle",
    )(*final)
    return jnp.transpose(moved, (1, 0, 2)), projected


def solution(mesh):
    in_specs = (
        P(("lat", "rad"), None, None),
        P(("lat", "rad"), None, None),
        P(None, ("lat", "rad")),
        P(("lat", "rad")),
        P(None, ("lat", "rad")),
        P(None, ("lat", "rad")),
    )
    out_specs = (P(("lat", "rad"), None, None), P(None, None, ("lat", "rad")))
    return jax.shard_map(
        functools.partial(per_device, mesh.shape["lat"], mesh.shape["rad"]),
        mesh=mesh, in_specs=in_specs, out_specs=out_specs, check_vma=False,
    )
```

```python
import functools
import itertools

import jax
import jax.numpy as jnp
from jax import lax
from jax.experimental import pallas as pl
from jax.experimental.pallas import tpu as pltpu
from jax.sharding import PartitionSpec as P

time_step = 0.4
MESH = pl.DeviceIdType.MESH
LANES = 128
bf16, f32, i32 = jnp.bfloat16, jnp.float32, jnp.int32


def round_up(x, by):
    return -(-x // by) * by


def split(x):
    high = x.astype(bf16)
    low = (x - high.astype(f32)).astype(bf16)
    return high, low


def dot(a, b, dims):
    return lax.dot_general(a, b, (dims, ((), ())), preferred_element_type=f32)


def iota(shape, axis):
    return lax.broadcasted_iota(i32, shape, axis)


def mask(condition):
    return condition.astype(f32).astype(bf16)


def lagrange(s):
    return (2.0 * (s - 0.5) * (s - 1.0), -4.0 * s * (s - 1.0), 2.0 * s * (s - 0.5))


def advance(points_in, coefficients, base, out, scale, group):
    markers = base.shape[1]

    def step(g, carry):
        rows = pl.ds(pl.multiple_of(g * group, group), group)
        lx = lagrange(points_in[0, rows, :])
        ly = lagrange(points_in[1, rows, :])
        lz = lagrange(points_in[2, rows, :])
        sums = [None] * 3
        for i in range(3):
            inner = [None] * 3
            for j in range(3):
                for c in range(3):
                    n = c * 27 + 9 * i + 3 * j
                    line = (
                        coefficients[n : n + 1, :] * lz[0]
                        + coefficients[n + 1 : n + 2, :] * lz[1]
                        + coefficients[n + 2 : n + 3, :] * lz[2]
                    ) * ly[j]
                    inner[c] = line if inner[c] is None else inner[c] + line
            for c in range(3):
                term = inner[c] * lx[i]
                sums[c] = term if sums[c] is None else sums[c] + term
        for c in range(3):
            out[c, rows, :] = base[c, rows, :] + scale * sums[c]
        return carry

    lax.fori_loop(0, markers // group, step, 0)


def parities(capacity):
    return ((0, 2), (1, 2)) if capacity % 2 == 0 else ((0, 1),)


def hits_of(tails, halves, count, owned, base):
    hits = []
    for index in range(len(halves)):
        at = index * (LANES // 2) + base
        element = tails[:, at : at + 1].astype(i32)
        hits.append(mask(iota((count, owned), 1) + 1 == element))
    return hits


def summed(lines, hits):
    total = None
    for line, hit in zip(lines, hits):
        high, low = split(line)
        part = dot(high, hit, ((1,), (0,))) + dot(low, hit, ((1,), (0,)))
        total = part if total is None else total + part
    return total


def trip(
    n_lat, n_rad, capacity,
    counts, pos_in, vel_in, elements_in, routes_in, fld_in,
    fin_t, fin_e, moved, early, inverse,
    pos, vel, elements, routes, raw, wide, carried,
    start_points, midway, landed, coef, phi, table,
    tab_a1, tab_a2, tab_t, tab_r, tab_e, tab_c, tab_m, first_t, second_t,
    points_m, midway_m, landed_m, coef_m0, coef_m1,
    request, asked, out_a1, in_a1, out_a2, in_a2, answer, answered, out_m,
    out_t, in_t, on_t, out_r, in_r, on_r, out_e, in_e, on_e, fin_m, fin_r, weights,
    index_v, turn_v, index_s, turn_s,
    load_sem, send_sem, recv_sem,
):
    lat, rad = lax.axis_index("lat"), lax.axis_index("rad")
    slots = 3 * n_rad
    places = slots * capacity
    shared = (capacity + 1) // 2
    together = max(n for n in range(1, 9) if slots % n == 0)
    groups = round_up(slots // together, 8)
    blocks, fields, markers = fld_in.shape
    n_vel, owned = vel.shape
    wide_places = points_m.shape[2]

    def load(index, source, target):
        copy = pltpu.make_async_copy(source, target, load_sem.at[index])
        copy.start()
        return copy

    load_routes = load(0, routes_in, routes)
    load_elements = load(1, elements_in, elements)
    load_pos = load(2, pos_in, pos)
    load_vel = load(3, vel_in, vel)
    load_fld = load(4, fld_in, raw)

    def partner(k, q, back):
        by = (1 - k) if back else (k - 1)
        return lax.rem(lat + by + n_lat, n_lat), q

    def outward(back):
        first = 2 * (2 * lat // n_lat)
        return enumerate((2 - first, first, 1) if back else (first, 2 - first, 1))

    barrier = pltpu.get_barrier_semaphore()
    for place, k in outward(False):

        def greet(dq, carry, k=k):
            q = lax.rem(rad + dq, n_rad)
            pl.semaphore_signal(
                barrier, inc=1, device_id=partner(k, q, False), device_id_type=MESH
            )
            return carry

        lax.fori_loop(int(place == 2), n_rad, greet, 0)

    def exchange(phase, source, target, size, back=False):
        for place, k in outward(back):

            def send(dq, carry, k=k, place=place):
                q = lax.rem(rad + dq, n_rad)
                if phase >= 10:
                    q = dq - 1 + (dq - 1 + n_rad - rad) // n_rad if place == 2 else dq
                pltpu.make_async_remote_copy(
                    src_ref=source.at[pl.ds((k * n_rad + q) * size, size)],
                    dst_ref=target.at[pl.ds((k * n_rad + rad) * size, size)],
                    send_sem=send_sem.at[phase],
                    recv_sem=recv_sem.at[phase],
                    device_id=partner(k, q, back),
                    device_id_type=MESH,
                ).start()
                return carry

            lax.fori_loop(int(place == 2), n_rad, send, 0)
        own = pl.ds((n_rad + rad) * size, size)
        pltpu.make_async_copy(source.at[own], target.at[own], recv_sem.at[phase]).start()

    def await_arrivals(phase, target, size):
        part = target.at[pl.ds(0, slots * size)]
        pltpu.make_async_copy(part, part, recv_sem.at[phase]).wait()

    def await_sends(phase, source, size):
        part = source.at[pl.ds(0, (slots - 1) * size)]
        pltpu.make_async_copy(part, part, send_sem.at[phase]).wait()

    def slot_of(place, each=capacity):
        return jnp.floor((place.astype(f32) + 0.5) * (1.0 / each)).astype(i32)

    def grouped(place):
        group = slot_of(place, capacity * together)
        return group, place - group * (capacity * together)

    def within(source, at, rows):
        bits = (source.shape[0] - rows + 1).bit_length() - 1
        return at & ((1 << bits) - 1)

    def place_rows(out, source, indices, row, rows):
        at_once = capacity * together

        def some(g, carry):
            for c in range(at_once):
                p = g * at_once + c
                at = within(source, indices[row * groups + g, c], rows)
                out[pl.ds(p * rows, rows), :] = source[pl.ds(at, rows), :]
            return carry

        lax.fori_loop(0, slots // together, some, 0)

    def place_tails(out, sources, indices):
        lower = iota((1, LANES), 1) < LANES // 2

        def some(g, carry):
            for s, pair in itertools.product(range(together), range(shared)):
                halves = []
                for half, source in enumerate(sources):
                    c = s * capacity + min(2 * pair + half, capacity - 1)
                    at = within(source, indices[g, c], 1)
                    halves.append(source[pl.ds(at, 1), :])
                line = jnp.where(lower, halves[0], halves[1])
                out[pl.ds((g * together + s) * shared + pair, 1), :] = line
            return carry

        lax.fori_loop(0, slots // together, some, 0)

    def clear(ref, start):
        ref[start:, :] = jnp.zeros((ref.shape[0] - start, LANES), f32)

    for ref, start in (
        (tab_a1, 2 * blocks), (tab_a2, 2 * blocks), (tab_t, blocks), (tab_r, blocks),
        (tab_e, 2 * blocks), (in_a1, 2 * places), (in_a2, 2 * places), (first_t, places),
        (second_t, places), (in_r, places), (in_e, 2 * places), (answer, 0), (coef, 0),
    ):
        clear(ref, start)
    index_v[...] = jnp.zeros(index_v.shape, i32)
    turn_v[...] = jnp.zeros(turn_v.shape, i32)

    load_routes.wait()
    load_elements.wait()
    route = jnp.where(iota((1, blocks), 1) < counts[0], routes[0:1, :], -1)
    slot = slot_of(route)
    sent_to = iota((slots, blocks), 0) == slot
    inside = mask(iota((LANES, blocks), 0) == route - slot * capacity)
    for row, label in enumerate((elements[1:2, :], routes[1:2, :])):
        marked = jnp.where(sent_to, (label + 1).astype(f32), 0.0).astype(bf16)
        request[:, row, :] = dot(marked, inside, ((1,), (1,)))
    group_of, within_group = grouped(route)
    chosen = iota((groups, blocks), 0) == group_of
    numbers = iota((groups, blocks), 1) - blocks
    numbers = jnp.where(chosen, numbers.astype(f32), 0.0).astype(bf16)
    matched = mask(iota((LANES, blocks), 0) == within_group)
    holder = (dot(numbers, matched, ((1,), (1,))) + float(blocks)).astype(i32)
    for row in range(2):
        index_v[row * groups : (row + 1) * groups, :] = holder * (1 << row)
    index_v[2 * groups : 2 * groups + 1, 0:blocks] = jnp.maximum(route, 0)
    indices = load(5, index_v, index_s)
    load_pos.wait()
    for c in range(2):
        tab_a1[pl.ds(c, blocks, stride=2), :] = pos[c]
    tab_a2[pl.ds(0, blocks, stride=2), :] = pos[2]
    indices.wait()
    place_rows(out_a1, tab_a1, index_s, 1, 2)
    pl.semaphore_wait(barrier, slots - 1)
    exchange(0, request, asked, 1)
    exchange(1, out_a1, in_a1, 2 * capacity)

    load_vel.wait()
    vel_high, vel_low = split(vel[...])
    pick = mask(iota((owned, blocks), 0) == elements[0:1, :])
    coef[0:n_vel, :] = dot(vel_high, pick, ((1,), (0,))) + dot(vel_low, pick, ((1,), (0,)))
    tab_a2[pl.ds(1, blocks, stride=2), :] = coef[...].T
    place_rows(out_a2, tab_a2, index_s, 1, 2)

    for c in range(3):
        start_points[c] = pos[c].T
    advance(start_points, coef, start_points, midway, 0.5 * time_step, 16)

    own_slot = slot_of(iota((places, slots), 0))
    by_slot = mask(own_slot == iota((places, slots), 1))
    lane = iota((places, LANES), 0) - slot_of(iota((places, LANES), 0)) * capacity
    by_lane = lane == iota((places, LANES), 1)

    def label_column(row):
        lines = dot(by_slot, asked[:, row, :].astype(bf16), ((1,), (0,)))
        return jnp.sum(jnp.where(by_lane, lines, 0.0), axis=1, keepdims=True).astype(i32)

    await_arrivals(0, asked, 1)
    pick = mask(iota((places, owned), 1) + 1 == label_column(0))
    answer[0:places, 0:n_vel] = dot(pick, vel_high, ((1,), (1,))) + dot(
        pick, vel_low, ((1,), (1,))
    )
    exchange(2, answer, answered, capacity, back=True)

    group_of, within_group = grouped(label_column(1) - 1)
    chosen = iota((places, LANES), 1) == group_of
    numbers = iota((places, LANES), 0) - places
    numbers = jnp.where(chosen, numbers.astype(f32), 0.0).astype(bf16)
    matched = mask(iota((places, LANES), 1) == within_group)
    holder = (dot(numbers, matched, ((0,), (0,))) + float(places)).astype(i32)
    for row in range(3):
        turn_v[row * groups : (row + 1) * groups, :] = holder[0:groups, :] * (1 << row)
    turns = load(6, turn_v, turn_s)
    load_fld.wait()
    wide[0 : blocks * fields, :] = raw[...].astype(f32).reshape(blocks * fields, markers)
    for f in range(fields):
        carried[pl.ds(f, markers, stride=fields), :] = wide[pl.ds(f, blocks, stride=fields), :].T

    exchange(3, out_a2, in_a2, 2 * capacity)

    await_arrivals(2, answered, capacity)

    for b in range(blocks):
        at = within(answered, index_s[2 * groups, b], 1)
        tab_c[b : b + 1, :] = answered[pl.ds(at, 1), :]
    coef[...] = tab_c[...].T
    advance(midway, coef, start_points, landed, time_step, 16)

    group = 8

    def basis(points, part, lanes, only=range(27)):
        lx = lagrange(points[0, part, lanes])
        ly = lagrange(points[1, part, lanes])
        lz = lagrange(points[2, part, lanes])
        for i, j in itertools.product(range(3), range(3)):
            nodes = [n for n in range(9 * i + 3 * j, 9 * i + 3 * j + 3) if n in only]
            if nodes:
                xy = lx[i] * ly[j]
                for n in nodes:
                    yield n, xy * lz[n % 3]

    def tabulate(only, group):
        def some(g, carry):
            part = pl.ds(pl.multiple_of(g * group, group), group)
            for n, value in basis(landed, part, slice(0, blocks), only):
                phi[n, part, :] = value
            return carry

        lax.fori_loop(0, markers // group, some, 0)

    def moments(nodes):
        def gather(g, sums):
            for s in range(8):
                m = g * 8 + s
                values = carried[pl.ds(pl.multiple_of(m * fields, fields), fields), :]
                sums = tuple(
                    total + phi[n, pl.ds(m, 1), :] * values for total, n in zip(sums, nodes)
                )
            return sums

        zero = jnp.zeros((fields, blocks), f32)
        sums = lax.fori_loop(0, markers // 8, gather, (zero,) * len(nodes))
        for index, total in enumerate(sums):
            table[index * fields : (index + 1) * fields, :] = total

    per_row = LANES // fields
    full = 27 // per_row
    last = tuple(range(full * per_row, 27))
    base = len(last) * fields
    half = LANES // 2
    tabulate(last, 32)
    moments(last)
    table[base:half, :] = jnp.zeros((half - base, blocks), f32)
    table[base : base + 1, :] = (elements[2:3, :] + 1).astype(f32)
    table[half:, :] = table[0:half, :]
    tab_t[0:blocks, :] = table[...].T
    place_tails(out_t, (tab_t, tab_t), index_s)
    exchange(4, out_t, in_t, shared)
    tabulate(range(full * per_row), group)
    moments(tuple(range(per_row)))
    tab_r[0:blocks, :] = table[...].T
    place_rows(out_r, tab_r, index_s, 0, 1)
    exchange(5, out_r, in_r, capacity)

    for j in range(2):
        moments(tuple(range((j + 1) * per_row, (j + 2) * per_row)))
        tab_e[pl.ds(j, blocks, stride=2), :] = table[...].T
    place_rows(out_e, tab_e, index_s, 1, 2)
    exchange(6, out_e, in_e, 2 * capacity)

    await_arrivals(1, in_a1, 2 * capacity)
    await_arrivals(3, in_a2, 2 * capacity)
    for part in range(wide_places // LANES):
        lanes = slice(part * LANES, (part + 1) * LANES)
        for c, (ref, row) in enumerate(((in_a1, 0), (in_a1, 1), (in_a2, 0))):
            points_m[c, :, lanes] = ref[pl.ds(2 * LANES * part + row, LANES, stride=2), :].T
        coef_m0[:, lanes] = in_a2[pl.ds(2 * LANES * part + 1, LANES, stride=2), :].T
        coef_m1[:, lanes] = answer[lanes, :].T
    advance(points_m, coef_m0, points_m, midway_m, 0.5 * time_step, 8)
    advance(midway_m, coef_m1, points_m, landed_m, time_step, 8)
    for part in range(wide_places // LANES):
        lanes = slice(part * LANES, (part + 1) * LANES)
        for c in range(3):
            tab_m[pl.ds(4 * LANES * part + c, LANES, stride=4), :] = landed_m[c, :, lanes].T
    turns.wait()
    place_rows(out_m, tab_m, turn_s, 2, 3)
    exchange(7, out_m, fin_m, 3 * capacity)

    await_arrivals(4, in_t, shared)
    tails = in_t[...]
    swapped = pltpu.roll(tails, half, 1)
    count = slots * shared
    for start, stride in parities(capacity):
        first_t[pl.ds(start, count, stride=stride), :] = swapped if start else tails
        second_t[pl.ds(start, count, stride=stride), :] = tails if start else swapped
    place_tails(on_t, (first_t, second_t), turn_s)
    exchange(8, on_t, fin_t, shared)
    await_arrivals(5, in_r, capacity)
    place_rows(on_r, in_r, turn_s, 0, 1)
    exchange(9, on_r, fin_r, capacity)
    await_arrivals(6, in_e, 2 * capacity)
    place_rows(on_e, in_e, turn_s, 1, 2)
    exchange(10, on_e, fin_e, 2 * capacity)

    await_arrivals(7, fin_m, 3 * capacity)
    halves = parities(capacity)
    count = places // len(halves)
    lanes_each = weights.shape[1] // len(halves)
    for index, (start, stride) in enumerate(halves):
        for c in range(3):
            tab_m[0:count, :] = fin_m[pl.ds(3 * start + c, count, stride=3 * stride), :]
            for part in range(lanes_each // LANES):
                at = index * lanes_each + part * LANES
                points_m[c, :, at : at + LANES] = tab_m[part * LANES : (part + 1) * LANES, :].T
    for part in range(weights.shape[1] // LANES):
        lanes = slice(part * LANES, (part + 1) * LANES)

        def square(g, sums, lanes=lanes):
            part = pl.ds(pl.multiple_of(g * group, group), group)
            return tuple(sums[n] + value * value for n, value in basis(points_m, part, lanes))

        zero = jnp.zeros((group, LANES), f32)
        sums = lax.fori_loop(0, markers // group, square, (zero,) * 27)
        for n in range(27):
            weights[n : n + 1, lanes] = jnp.sum(sums[n], axis=0, keepdims=True)
        weights[27:, lanes] = jnp.zeros((weights.shape[0] - 27, LANES), f32)

    for c in range(3):
        moved[c] = fin_m[pl.ds(c, places, stride=3), :]
    await_arrivals(8, fin_t, shared)
    hits = hits_of(fin_t, halves, places // len(halves), owned, base)
    sums = summed(
        [weights[:, at * lanes_each : at * lanes_each + count] for at in range(len(halves))], hits
    )
    inverse[...] = 1.0 / (1.0 + sums)
    turned = fin_t[...].T
    sums = summed([turned[at * half : (at + 1) * half] for at in range(len(halves))], hits)
    for n in range(len(last)):
        node = full * per_row + n
        early[per_row + n] = sums[n * fields : (n + 1) * fields] * inverse[node : node + 1, :]
    await_arrivals(9, fin_r, capacity)
    sums = summed([fin_r[pl.ds(start, count, stride=stride), :].T for start, stride in halves], hits)
    for n in range(per_row):
        early[n] = sums[n * fields : (n + 1) * fields] * inverse[n : n + 1, :]

    await_arrivals(10, fin_e, 2 * capacity)
    await_sends(0, request, 1)
    await_sends(1, out_a1, 2 * capacity)
    await_sends(2, answer, capacity)
    await_sends(3, out_a2, 2 * capacity)
    await_sends(4, out_t, shared)
    await_sends(5, out_r, capacity)
    await_sends(6, out_e, 2 * capacity)
    await_sends(7, out_m, 3 * capacity)
    await_sends(8, on_t, shared)
    await_sends(9, on_r, capacity)
    await_sends(10, on_e, 2 * capacity)


def settle(
    fields, places, base, halves, tails, rest, moved, early, inverse, moved_out, projected_out,
    projected, sems,
):
    owned = projected.shape[2]
    per_row = LANES // fields
    n_late = projected.shape[0]

    def write(index, source, target):
        copy = pltpu.make_async_copy(source, target, sems.at[index])
        copy.start()
        return copy

    n_last = early.shape[0] - per_row
    copies = [
        write(0, early.at[pl.ds(0, per_row)], projected_out.at[pl.ds(0, per_row)]),
        write(1, early.at[pl.ds(per_row, n_last)], projected_out.at[pl.ds(per_row + n_late, n_last)]),
        write(2, moved, moved_out),
    ]
    count = places // len(halves)
    hits = hits_of(tails, halves, count, owned, base)
    for j in range(n_late // per_row):
        sums = summed(
            [rest[pl.ds(2 * start + j, count, stride=2 * stride), :].T for start, stride in halves],
            hits,
        )
        for n in range(per_row):
            node = (j + 1) * per_row + n
            projected[j * per_row + n] = (
                sums[n * fields : (n + 1) * fields, :] * inverse[node : node + 1, :]
            )
        copies.append(
            write(
                3 + j,
                projected.at[pl.ds(j * per_row, per_row)],
                projected_out.at[pl.ds((j + 1) * per_row, per_row)],
            )
        )
    for copy in copies:
        copy.wait()


def per_device(n_lat, n_rad, positions, fields, velocity, counts, elements, routes):
    blocks, _, markers = positions.shape
    n_fields = fields.shape[1]
    capacity = max(1, 2 * blocks // (3 * n_rad))
    slots = 3 * n_rad
    places = slots * capacity
    shared = slots * ((capacity + 1) // 2)
    owned = velocity.shape[1]
    wide_places = round_up(places + 1, LANES)
    halves = len(parities(capacity))
    weight_lanes = halves * round_up(places // halves, LANES)
    vmem = pl.BlockSpec(memory_space=pltpu.VMEM)
    anywhere = pl.BlockSpec(memory_space=pltpu.HBM)

    def rows(n):
        return pltpu.VMEM((round_up(n, 8), LANES), f32)

    def looked_up(n, each):
        return rows((1 << (n * each).bit_length()) + each)

    small = pltpu.VMEM((slots, 2, LANES), f32)
    points = pltpu.VMEM((3, markers, blocks), f32)
    wide_points = pltpu.VMEM((3, markers, wide_places), f32)
    square = pltpu.VMEM((LANES, LANES), f32)
    together = max(n for n in range(1, 9) if slots % n == 0)
    index_rows = 3 * round_up(slots // together, 8)
    index = pltpu.VMEM((index_rows, LANES), i32)
    index_s = pltpu.SMEM((index_rows, LANES), i32)
    per_row = LANES // n_fields
    n_last = 27 % per_row
    inputs = (jnp.transpose(positions, (1, 0, 2)), velocity, elements, routes, fields)
    final = pl.pallas_call(
        functools.partial(trip, n_lat, n_rad, capacity),
        out_shape=[
            jax.ShapeDtypeStruct(shape, f32)
            for shape in (
                (shared, LANES), (2 * places, LANES), (3, places, markers),
                (per_row + n_last, n_fields, owned), (32, owned),
            )
        ],
        in_specs=[pl.BlockSpec(memory_space=pltpu.SMEM)] + [anywhere] * 5,
        out_specs=[vmem] * 5,
        scratch_shapes=[
            pltpu.VMEM((3, blocks, markers), f32),
            pltpu.VMEM(velocity.shape, f32),
            pltpu.VMEM(elements.shape, i32),
            pltpu.VMEM(routes.shape, i32),
            pltpu.VMEM(fields.shape, fields.dtype),
            rows((blocks + 1) * n_fields), rows((markers + 1) * n_fields),
            points, points, points,
            square,
            pltpu.VMEM((27, markers, blocks), f32),
            square,
            looked_up(blocks, 2), looked_up(blocks, 2),
            looked_up(blocks, 1), looked_up(blocks, 1), looked_up(blocks, 2),
            square, looked_up(wide_places - 1, 4),
            looked_up(places, 1), looked_up(places, 1),
            wide_points, wide_points, wide_points,
            pltpu.VMEM((LANES, wide_places), f32), pltpu.VMEM((LANES, wide_places), f32),
            small, small,
            rows(2 * places), rows(2 * wide_places + 8),
            rows(2 * places), rows(2 * wide_places + 8),
            rows(wide_places), looked_up(places, 1), rows(3 * places),
            rows(shared), rows(shared), rows(shared),
            rows(places), looked_up(places, 1), rows(places),
            rows(2 * places), looked_up(places, 2), rows(2 * places),
            rows(3 * places), rows(places), pltpu.VMEM((32, weight_lanes), f32),
            index, index, index_s, index_s,
            pltpu.SemaphoreType.DMA((8,)),
            pltpu.SemaphoreType.DMA((11,)),
            pltpu.SemaphoreType.DMA((11,)),
        ],
        compiler_params=pltpu.CompilerParams(
            collective_id=0, has_side_effects=True, vmem_limit_bytes=24 * 1024 * 1024
        ),
        name="trip",
    )(counts, *[pltpu.with_memory_space_constraint(x, pltpu.HBM) for x in inputs])
    moved, projected = pl.pallas_call(
        functools.partial(settle, n_fields, places, n_last * n_fields, parities(capacity)),
        out_shape=(
            jax.ShapeDtypeStruct((3, places, markers), f32),
            jax.ShapeDtypeStruct((27, n_fields, owned), f32),
        ),
        in_specs=[vmem] * 5,
        out_specs=(anywhere, anywhere),
        scratch_shapes=[
            pltpu.VMEM((27 - per_row - n_last, n_fields, owned), f32),
            pltpu.SemaphoreType.DMA((27 // per_row + 2,)),
        ],
        compiler_params=pltpu.CompilerParams(vmem_limit_bytes=16 * 1024 * 1024),
        name="settle",
    )(*final)
    return jnp.transpose(moved, (1, 0, 2)), projected


def solution(mesh):
    in_specs = (
        P(("lat", "rad"), None, None),
        P(("lat", "rad"), None, None),
        P(None, ("lat", "rad")),
        P(("lat", "rad")),
        P(None, ("lat", "rad")),
        P(None, ("lat", "rad")),
    )
    out_specs = (P(("lat", "rad"), None, None), P(None, None, ("lat", "rad")))
    return jax.shard_map(
        functools.partial(per_device, mesh.shape["lat"], mesh.shape["rad"]),
        mesh=mesh, in_specs=in_specs, out_specs=out_specs, check_vma=False,
    )
```
